32 devices in a mesh: replica: 1 (over z), model: 32 (over y, x, core).
Axes of the slice: x: 4, y: 4, z: 1, core: 2. Of those that a mesh axis runs over, the one named last changes fastest.
The devices are a block of a 4x4x8 slice.
Arguments:
- hidden: bfloat16 [2048, 8192], P('replica')
- w_query: bfloat16 [8192, 8192], P(None, 'model')
- w_key: bfloat16 [8192, 128], replicated
- w_value: bfloat16 [8192, 128], replicated
- w_out: bfloat16 [8192, 8192], P('model')
- key_cache: bfloat16 [2048, 512, 128], P(('replica', 'model'))
- value_cache: bfloat16 [2048, 512, 128], P(('replica', 'model'))
- lengths: int32 [2048], P('replica')
Outputs:
- output 1: bfloat16 [2048, 8192], P('replica')
- output 2: bfloat16 [2048, 512, 128], P(('replica', 'model'))
- output 3: bfloat16 [2048, 512, 128], P(('replica', 'model'))
All inputs are finite; a program needn't handle non-finite values.
Results may differ from the reference program's by a relative error of at most 0.0109961.
Values are sent between devices in bfloat16 or wider.
A program may use at most 768 MiB of HBM per device.

```python
import math
import jax
import jax.numpy as jnp
from jax import lax

MODEL_DIM = 8192
QUERY_HEADS = 64
HEAD_DIM = 128
SEQ_LEN = 512
BATCH_ROWS = 2048
LOG_SEQ = int(math.log2(SEQ_LEN))


def draw_cache_row(row_key):
    return jax.random.normal(row_key, (SEQ_LEN, HEAD_DIM), jnp.float32).astype(jnp.bfloat16)


def draw_lengths(len_keys):
    len_exponent = jax.random.randint(len_keys[0], (BATCH_ROWS,), 0, LOG_SEQ + 1)
    upper_len = jnp.left_shift(jnp.ones_like(len_exponent), len_exponent)
    lower_len = upper_len // 2
    drawn_len = jax.random.randint(len_keys[1], (BATCH_ROWS,), lower_len, upper_len)
    top_row = jax.random.randint(len_keys[2], (), 0, BATCH_ROWS)
    return jnp.where(jnp.arange(BATCH_ROWS) == top_row, SEQ_LEN - 1, drawn_len).astype(jnp.int32)


def setup_inputs(seed: int = 0, part: int = 0) -> dict:
    base_key = jax.random.key(seed)
    shared_keys = jax.random.split(base_key, 4)
    part_keys = jax.random.split(jax.random.fold_in(base_key, part), 6)
    query_width = QUERY_HEADS * HEAD_DIM
    hidden = jax.random.normal(part_keys[0], (BATCH_ROWS, MODEL_DIM), jnp.float32)
    w_query = jax.random.normal(shared_keys[0], (MODEL_DIM, query_width), jnp.float32) * (3.0 / math.sqrt(MODEL_DIM))
    w_key = jax.random.normal(shared_keys[1], (MODEL_DIM, HEAD_DIM), jnp.float32) / math.sqrt(MODEL_DIM)
    w_value = jax.random.normal(shared_keys[2], (MODEL_DIM, HEAD_DIM), jnp.float32) / math.sqrt(MODEL_DIM)
    w_out = jax.random.normal(shared_keys[3], (query_width, MODEL_DIM), jnp.float32) / math.sqrt(query_width)
    key_cache = lax.map(draw_cache_row, jax.random.split(part_keys[1], BATCH_ROWS))
    value_cache = lax.map(draw_cache_row, jax.random.split(part_keys[2], BATCH_ROWS))
    lengths = draw_lengths(part_keys[3:6])
    return {'hidden': hidden.astype(jnp.bfloat16), 'w_query': w_query.astype(jnp.bfloat16), 'w_key': w_key.astype(jnp.bfloat16), 'w_value': w_value.astype(jnp.bfloat16), 'w_out': w_out.astype(jnp.bfloat16), 'key_cache': key_cache, 'value_cache': value_cache, 'lengths': lengths}


def attend_row(row_args):
    query_row, key_row, value_row, row_len = row_args
    scores = jnp.einsum('hd,td->ht', query_row.astype(jnp.float32), key_row.astype(jnp.float32)) * (HEAD_DIM ** -0.5)
    valid_pos = jnp.arange(SEQ_LEN)[None, :] <= row_len
    scores = jnp.where(valid_pos, scores, -jnp.inf)
    weights = jnp.exp(scores - jnp.max(scores, axis=1, keepdims=True))
    weight_sum = jnp.sum(weights, axis=1)
    weighted_sum = jnp.einsum('ht,td->hd', weights.astype(jnp.bfloat16).astype(jnp.float32), value_row.astype(jnp.float32))
    return (weighted_sum / weight_sum[:, None]).astype(jnp.bfloat16)


def reference(hidden, w_query, w_key, w_value, w_out, key_cache, value_cache, lengths):
    query = jnp.dot(hidden, w_query, preferred_element_type=jnp.float32).astype(jnp.bfloat16)
    query = query.reshape(BATCH_ROWS, QUERY_HEADS, HEAD_DIM)
    key_new = jnp.dot(hidden, w_key, preferred_element_type=jnp.float32).astype(jnp.bfloat16)
    value_new = jnp.dot(hidden, w_value, preferred_element_type=jnp.float32).astype(jnp.bfloat16)
    write_pos = jnp.arange(SEQ_LEN)[None, :, None] == lengths[:, None, None]
    key_upd = jnp.where(write_pos, key_new[:, None, :], key_cache)
    value_upd = jnp.where(write_pos, value_new[:, None, :], value_cache)
    context = lax.map(attend_row, (query, key_upd, value_upd, lengths))
    attn_out = jnp.dot(context.reshape(BATCH_ROWS, QUERY_HEADS * HEAD_DIM), w_out, preferred_element_type=jnp.float32)
    hidden_out = (hidden.astype(jnp.float32) + attn_out).astype(jnp.bfloat16)
    return (hidden_out, key_upd, value_upd)
```

```python
import functools
import math
import jax
import jax.numpy as jnp
from jax import lax
from jax.experimental import pallas as pl
from jax.experimental.pallas import tpu as pltpu
from jax.sharding import PartitionSpec as P

ROWS_PER_STEP = 4


def attend_kernel(len_ref, q_ref, kn_ref, vn_ref, k_ref, v_ref, ko_ref, vo_ref, ctx_ref):
    rows, seq_len, head_dim = k_ref.shape
    n_heads = q_ref.shape[1]
    scale = head_dim ** -0.5
    step = pl.program_id(0)
    tile = math.gcd(seq_len, 16)
    ko_ref[...] = k_ref[...]
    vo_ref[...] = v_ref[...]
    spans = [s for s in (128, 256) if s < seq_len] + [seq_len]
    for r in range(rows):
        row_len = len_ref[step * rows + r]
        base = pl.multiple_of((row_len // tile) * tile, tile)
        pick = lax.broadcasted_iota(jnp.int32, (tile, head_dim), 0) == row_len - base
        for new_ref, out_ref in ((kn_ref, ko_ref), (vn_ref, vo_ref)):
            new = jnp.broadcast_to(new_ref[0, r:r + 1, :], (tile, head_dim)).astype(jnp.float32)
            old = out_ref[r, pl.ds(base, tile), :].astype(jnp.float32)
            out_ref[r, pl.ds(base, tile), :] = jnp.where(pick, new, old).astype(jnp.bfloat16)
        lower = 0
        for span in spans:
            @pl.when((row_len >= lower) & (row_len < span))
            def _(span=span):
                s = lax.dot_general(q_ref[r], ko_ref[r, :span, :], (((1,), (1,)), ((), ())), preferred_element_type=jnp.float32) * scale
                pos = lax.broadcasted_iota(jnp.int32, (n_heads, span), 1)
                s = jnp.where(pos <= row_len, s, -jnp.inf)
                e = jnp.exp(s - jnp.max(s, axis=1, keepdims=True))
                total = jnp.sum(e, axis=1, keepdims=True)
                acc = jnp.dot(e.astype(jnp.bfloat16), vo_ref[r, :span, :], preferred_element_type=jnp.float32)
                ctx_ref[r] = (acc / total).astype(jnp.bfloat16)
            lower = span


def attend(lens, query, key_new, value_new, key_cache, value_cache):
    n, seq_len, head_dim = key_cache.shape
    n_heads = query.shape[1]
    rows = math.gcd(n, ROWS_PER_STEP)
    cache = pl.BlockSpec((rows, seq_len, head_dim), lambda i, lens: (i, 0, 0))
    new = pl.BlockSpec((1, rows, head_dim), lambda i, lens: (i, 0, 0))
    heads = pl.BlockSpec((rows, n_heads, head_dim), lambda i, lens: (i, 0, 0))
    return pl.pallas_call(
        attend_kernel,
        grid_spec=pltpu.PrefetchScalarGridSpec(
            num_scalar_prefetch=1,
            grid=(n // rows,),
            in_specs=[heads, new, new, cache, cache],
            out_specs=[cache, cache, heads],
        ),
        out_shape=[
            jax.ShapeDtypeStruct(key_cache.shape, key_cache.dtype),
            jax.ShapeDtypeStruct(value_cache.shape, value_cache.dtype),
            jax.ShapeDtypeStruct(query.shape, jnp.bfloat16),
        ],
        cost_estimate=pl.CostEstimate(flops=4 * n * n_heads * seq_len * head_dim, bytes_accessed=8 * n * seq_len * head_dim, transcendentals=0),
        name='attend',
    )(lens, query, key_new.reshape(n // rows, rows, head_dim), value_new.reshape(n // rows, rows, head_dim), key_cache, value_cache)


def solution(mesh):
    def group_step(hidden, w_query, w_key, w_value, w_out, key_cache, value_cache, lengths):
        n_rows = hidden.shape[0]
        local_rows = key_cache.shape[0]
        head_dim = key_cache.shape[2]
        local_heads = w_query.shape[1] // head_dim
        row_start = lax.axis_index('model') * local_rows
        query = jnp.dot(hidden, w_query, preferred_element_type=jnp.float32).astype(jnp.bfloat16)
        query = query.reshape(n_rows, local_heads, head_dim)
        query_local = lax.all_to_all(query, 'model', 0, 1, tiled=True)
        hidden_local = lax.dynamic_slice_in_dim(hidden, row_start, local_rows, 0)
        len_local = lax.dynamic_slice_in_dim(lengths, row_start, local_rows, 0)
        key_new = jnp.dot(hidden_local, w_key, preferred_element_type=jnp.float32).astype(jnp.bfloat16)
        value_new = jnp.dot(hidden_local, w_value, preferred_element_type=jnp.float32).astype(jnp.bfloat16)
        key_upd, value_upd, context = attend(len_local, query_local, key_new, value_new, key_cache, value_cache)
        context_back = lax.all_to_all(context, 'model', 1, 0, tiled=True)
        part_sum = jnp.dot(context_back.reshape(n_rows, local_heads * head_dim), w_out, preferred_element_type=jnp.float32).astype(jnp.bfloat16)
        attn_out = lax.psum(part_sum, 'model')
        hidden_out = (hidden.astype(jnp.float32) + attn_out.astype(jnp.float32)).astype(jnp.bfloat16)
        return hidden_out, key_upd, value_upd

    row_spec = P('replica', None)
    cache_spec = P(('replica', 'model'), None, None)
    return jax.shard_map(group_step, mesh=mesh, in_specs=(row_spec, P(None, 'model'), P(None, None), P(None, None), P('model', None), cache_spec, cache_spec, P('replica')), out_specs=(row_spec, cache_spec, cache_spec), check_vma=False)
```

```python
import functools
import math
import jax
import jax.numpy as jnp
from jax import lax
from jax.experimental import pallas as pl
from jax.experimental.pallas import tpu as pltpu
from jax.sharding import PartitionSpec as P

ROWS_PER_STEP = 4


def attend_kernel(len_ref, q_ref, kn_ref, vn_ref, k_ref, v_ref, ko_ref, vo_ref, ctx_ref):
    rows, seq_len, head_dim = k_ref.shape
    n_heads = q_ref.shape[1]
    scale = head_dim ** -0.5
    step = pl.program_id(0)
    tile = math.gcd(seq_len, 16)
    ko_ref[...] = k_ref[...]
    vo_ref[...] = v_ref[...]
    spans = [s for s in (128, 256) if s < seq_len] + [seq_len]
    for r in range(rows):
        row_len = len_ref[step * rows + r]
        base = pl.multiple_of((row_len // tile) * tile, tile)
        pick = lax.broadcasted_iota(jnp.int32, (tile, head_dim), 0) == row_len - base
        for new_ref, out_ref in ((kn_ref, ko_ref), (vn_ref, vo_ref)):
            new = jnp.broadcast_to(new_ref[0, r:r + 1, :], (tile, head_dim)).astype(jnp.float32)
            old = out_ref[r, pl.ds(base, tile), :].astype(jnp.float32)
            out_ref[r, pl.ds(base, tile), :] = jnp.where(pick, new, old).astype(jnp.bfloat16)
        lower = 0
        for span in spans:
            @pl.when((row_len >= lower) & (row_len < span))
            def _(span=span):
                s = lax.dot_general(q_ref[r], ko_ref[r, :span, :], (((1,), (1,)), ((), ())), preferred_element_type=jnp.float32) * scale
                pos = lax.broadcasted_iota(jnp.int32, (n_heads, span), 1)
                s = jnp.where(pos <= row_len, s, -jnp.inf)
                e = jnp.exp(s - jnp.max(s, axis=1, keepdims=True))
                total = jnp.sum(e, axis=1, keepdims=True)
                acc = jnp.dot(e.astype(jnp.bfloat16), vo_ref[r, :span, :], preferred_element_type=jnp.float32)
                ctx_ref[r] = (acc / total).astype(jnp.bfloat16)
            lower = span


def attend(lens, query, key_new, value_new, key_cache, value_cache):
    n, seq_len, head_dim = key_cache.shape
    n_heads = query.shape[1]
    rows = math.gcd(n, ROWS_PER_STEP)
    cache = pl.BlockSpec((rows, seq_len, head_dim), lambda i, lens: (i, 0, 0))
    new = pl.BlockSpec((1, rows, head_dim), lambda i, lens: (i, 0, 0))
    heads = pl.BlockSpec((rows, n_heads, head_dim), lambda i, lens: (i, 0, 0))
    return pl.pallas_call(
        attend_kernel,
        grid_spec=pltpu.PrefetchScalarGridSpec(
            num_scalar_prefetch=1,
            grid=(n // rows,),
            in_specs=[heads, new, new, cache, cache],
            out_specs=[cache, cache, heads],
        ),
        out_shape=[
            jax.ShapeDtypeStruct(key_cache.shape, key_cache.dtype),
            jax.ShapeDtypeStruct(value_cache.shape, value_cache.dtype),
            jax.ShapeDtypeStruct(query.shape, jnp.bfloat16),
        ],
        cost_estimate=pl.CostEstimate(flops=4 * n * n_heads * seq_len * head_dim, bytes_accessed=8 * n * seq_len * head_dim, transcendentals=0),
        name='attend',
    )(lens, query, key_new.reshape(n // rows, rows, head_dim), value_new.reshape(n // rows, rows, head_dim), key_cache, value_cache)


MESH = pl.DeviceIdType.MESH
CORES = 2


class Moves:
    def __init__(self, send_sems, recv_sems):
        self.send_sems, self.recv_sems = send_sems, recv_sems
        self.count, self.copies, self.unsent = 0, {}, []

    def send(self, key, src, dst, device):
        copy = pltpu.make_async_remote_copy(src_ref=src, dst_ref=dst, send_sem=self.send_sems.at[self.count], recv_sem=self.recv_sems.at[self.count], device_id={'model': device}, device_id_type=MESH)
        copy.start()
        self.count += 1
        self.copies[key] = copy
        self.unsent.append(copy)

    def local(self, key, src, dst):
        copy = pltpu.make_async_copy(src, dst, self.send_sems.at[self.count])
        copy.start()
        self.count += 1
        self.copies[key] = copy

    def got(self, key):
        self.copies.pop(key).wait_recv()

    def done(self, key):
        self.copies.pop(key).wait()

    def finish(self):
        for copy in self.unsent:
            copy.wait_send()


def place(side):
    me = lax.axis_index('model')
    return me // (CORES * side), lax.rem(me // CORES, side), lax.rem(me, CORES)


def greet(devices):
    barrier = pltpu.get_barrier_semaphore()
    for device in devices:
        pl.semaphore_signal(barrier, inc=1, device_id={'model': device}, device_id_type=MESH)
    pl.semaphore_wait(barrier, len(devices))


def columns(start, width):
    return pl.ds(pl.multiple_of(start * width, width), width)


def query_kernel(side, hid_ref, wq_ref, wo_ref, q_ref, wa_ref, wb_ref, wq_all, hid, q_buf, acc, relay, own_w, send_sems, recv_sems):
    y, x, c = place(side)
    rows, dim = hid_ref.shape[3:]
    half = wq_ref.shape[1]
    w_rows = wo_ref.shape[0]
    width = wo_ref.shape[1] // (2 * side)
    w_refs = (wa_ref, wb_ref)
    step = lambda a, d: lax.rem(a + d + side, side)
    dev = lambda yy, xx: (yy * side + xx) * CORES + c
    other = (y * side + x) * CORES + 1 - c
    peers = [(dy, dx) for dy in range(side) for dx in range(side) if dy or dx]
    greet([dev(step(y, dy), step(x, dx)) for dy, dx in peers] + [other])
    mv = Moves(send_sems, recv_sems)
    order = list(range(1, side)) + [0]
    mv.send('wq', wq_ref, wq_all.at[c], other)
    mv.local('wq_own', wq_ref, wq_all.at[c])
    for i, dy in enumerate(order):
        mv.local(('hid', i), hid_ref.at[step(y, dy), :, c], hid.at[i])
    along = ((x, lambda u: dev(y, u)), (y, lambda u: dev(u, x)))
    wcols = lambda t, u: columns(t * side + u, width)
    top, low = pl.ds(0, w_rows // 2), pl.ds(w_rows // 2, w_rows // 2)
    for t, (u, at) in enumerate(along):
        mv.send(('w1R', t), wo_ref.at[top, wcols(t, step(u, 2))], relay.at[t, 0], at(step(u, 1)))
        mv.send(('w1L', t), wo_ref.at[low, wcols(t, step(u, 2))], relay.at[t, 1], at(step(u, -1)))
        mv.local(('w_own', t), wo_ref.at[:, wcols(t, u)], own_w.at[t])
    for t, (u, at) in enumerate(along):
        mv.send(('wR', t), wo_ref.at[:, wcols(t, step(u, 1))], w_refs[t].at[u, c], at(step(u, 1)))
        mv.send(('wL', t), wo_ref.at[:, wcols(t, step(u, -1))], w_refs[t].at[u, c], at(step(u, -1)))
        mv.send(('wS', t, 0), wo_ref.at[:, wcols(t, u)], w_refs[t].at[u, c], other)

    depth = min(1024, dim)

    def project(i, core):
        acc[...] = jnp.zeros_like(acc)

        @pl.loop(0, dim // depth)
        def _(k):
            part = columns(k, depth)
            acc[...] += jnp.dot(hid[i, :, :, part].reshape(side * rows, depth), wq_all[core, part, :], preferred_element_type=jnp.float32)

        q_buf[i, :, :, columns(core, half)] = acc[...].astype(jnp.bfloat16).reshape(side, rows, half)

    mv.done('wq_own')
    for i in range(side):
        mv.done(('hid', i))
        project(i, c)
    for t, (u, at) in enumerate(along):
        mv.done(('w_own', t))
        mv.local(('w_put', t), own_w.at[t], w_refs[t].at[u, c])
        mv.got(('w1R', t))
        mv.send(('w2R', t), relay.at[t, 0], w_refs[t].at[step(u, -1), c, top], at(step(u, 1)))
        mv.got(('w1L', t))
        mv.send(('w2L', t), relay.at[t, 1], w_refs[t].at[step(u, 1), c, low], at(step(u, -1)))
    mv.got('wq')
    for i, dy in enumerate(order):
        project(i, 1 - c)
        for dx in [d for d in (2, 1, 3, 0)][:side]:
            if dy or dx:
                mv.send(('q', dy, dx), q_buf.at[i, step(x, dx)], q_ref.at[y, x], dev(step(y, dy), step(x, dx)))
            else:
                mv.local('q_own', q_buf.at[i, x], q_ref.at[y, x])
    for t, (u, at) in enumerate(along):
        mv.got(('wR', t))
        mv.send(('wS', t, 1), w_refs[t].at[step(u, -1), c], w_refs[t].at[step(u, -1), c], other)
        mv.got(('wL', t))
        mv.send(('wS', t, 3), w_refs[t].at[step(u, 1), c], w_refs[t].at[step(u, 1), c], other)
    for t, (u, at) in enumerate(along):
        mv.got(('w2R', t))
        mv.got(('w2L', t))
        mv.send(('wS', t, 2), w_refs[t].at[step(u, 2), c], w_refs[t].at[step(u, 2), c], other)
    for dy, dx in peers:
        mv.got(('q', dy, dx))
    mv.done('q_own')
    for t in range(2):
        mv.done(('w_put', t))
        for d in range(side):
            mv.got(('wS', t, d))
    mv.finish()


def output_kernel(side, ctx_ref, wa_ref, wb_ref, hid_ref, out_ref, held, w_buf, hid, acc, part, first, second, final, send_sems, recv_sems):
    y, x, c = place(side)
    rows, depth = ctx_ref.shape[2:]
    width = w_buf.shape[-1]
    step = lambda a, d: lax.rem(a + d + side, side)
    dev = lambda yy, xx: (yy * side + xx) * CORES + c
    other = (y * side + x) * CORES + 1 - c
    spots = ((y, x), (x, y))
    at = lambda t, v, u: dev(v, u) if t == 0 else dev(u, v)
    ctx_of = lambda t, v: ctx_ref.at[v] if t == 0 else ctx_ref.at[:, v]
    greet([dev(y, step(x, d)) for d in range(1, side)] + [dev(step(y, d), x) for d in range(1, side)] + [other])
    mv = Moves(send_sems, recv_sems)
    both = range(2)

    def view(ref, t, v, g, us=None):
        us = slice(None) if us is None else us
        cols = columns(t * side + g, width)
        return ref.at[v, us, c, :, cols] if t == 0 else ref.at[us, v, c, :, cols]

    for t in both:
        v, u = spots[t]
        mv.send(('a', t, 2), ctx_of(t, step(v, 2)), held.at[t, u, v], at(t, step(v, 2), u))
    for t in both:
        v, u = spots[t]
        for d in (1, 3):
            mv.send(('a', t, d), ctx_of(t, step(v, d)), held.at[t, u, v], at(t, step(v, d), u))
        mv.send(('gR', t, 0), ctx_of(t, v), held.at[t, u, v], at(t, v, step(u, 1)))
        mv.send(('gL', t, 0), ctx_of(t, v), held.at[t, u, v], at(t, v, step(u, -1)))
    for t in both:
        v, u = spots[t]
        mv.local(('w', t), (wa_ref, wb_ref)[t], w_buf.at[t])
        mv.local(('hid', t), view(hid_ref, t, v, u), hid.at[t])
    for p in (1, 3, 2):
        for t in both:
            v, u = spots[t]
            mv.got(('a', t, p))
            slot = held.at[t, u, step(v, -p)]
            mv.send(('gR', t, p), slot, slot, at(t, v, step(u, 1)))
            mv.send(('gL', t, p), slot, slot, at(t, v, step(u, -1)))
    for p in (0, 1, 3, 2):
        for t in both:
            v, u = spots[t]
            mv.got(('gR', t, p))
            if p in (0, 2):
                slot = held.at[t, step(u, -1), step(v, -p)]
                mv.send(('f', t, p), slot, slot, at(t, v, step(u, 1)))
            mv.got(('gL', t, p))
            if p in (1, 3):
                slot = held.at[t, step(u, 1), step(v, -p)]
                mv.send(('f', t, p), slot, slot, at(t, v, step(u, -1)))
    for t in both:
        mv.done(('w', t))

    def product(t, p):
        v, u = spots[t]
        total = None
        for k in range(side):
            pieces = []
            for d in range(side):
                if p == 0 and d == 0:
                    pieces.append(ctx_ref[v, k] if t == 0 else ctx_ref[k, v])
                else:
                    pieces.append(held[t, step(u, d), step(v, -p), k])
            one = jnp.dot(jnp.concatenate(pieces, axis=0), w_buf[t, k].reshape(depth, width), preferred_element_type=jnp.float32)
            total = one if total is None else total + one
        acc[t] = total.reshape(side, rows, width)

    upper, lower = pl.ds(0, side // 2), pl.ds(side // 2, side // 2)
    for t in both:
        v, u = spots[t]
        mv.got(('f', t, 2))
        product(t, 2)
        part[t, 2] = acc[t].astype(jnp.bfloat16)
        mv.send(('r1R', t), part.at[t, 2, upper], first.at[t, 0], at(t, step(v, 1), u))
        mv.send(('r1L', t), part.at[t, 2, lower], first.at[t, 1], at(t, step(v, -1), u))
    for p, now, later, tag, d in ((1, upper, lower, 'L', 1), (3, lower, upper, 'R', 0)):
        for t in both:
            v, u = spots[t]
            to = at(t, step(v, -p), u)
            mv.got(('f', t, p))
            product(t, p)
            part[t, p, now] = acc[t, now].astype(jnp.bfloat16)
            mv.send(('r2' + tag, t), part.at[t, p, now], second.at[t, d, now], to)
            mv.got(('r1' + tag, t))
            part[t, p, later] = (acc[t, later] + first[t, d].astype(jnp.float32)).astype(jnp.bfloat16)
            mv.send(('r3' + tag, t), part.at[t, p, later], second.at[t, d, later], to)
    for t in both:
        mv.got(('f', t, 0))
        product(t, 0)
    for t in both:
        v, u = spots[t]
        for tag in 'RL':
            mv.got(('r2' + tag, t))
            mv.got(('r3' + tag, t))
        mv.done(('hid', t))
        for d in range(side):
            us = step(u, d)
            y_sum = acc[t, d] + second[t, 0, d].astype(jnp.float32) + second[t, 1, d].astype(jnp.float32)
            final[t, us] = (hid[t, us].astype(jnp.float32) + y_sum).astype(jnp.bfloat16)
        mine = view(out_ref, t, v, u)
        mv.send(('oR', t), final.at[t], mine, at(t, v, step(u, 1)))
        mv.send(('oL', t), final.at[t], mine, at(t, v, step(u, -1)))
        mv.send(('pR', t, 0), final.at[t], mine, at(t, step(v, 1), u))
        mv.send(('pL', t, 0), final.at[t], mine, at(t, step(v, -1), u))
        mv.local(('own', t), final.at[t], mine)
        mv.send(('s', t, 0, 0), final.at[t], mine, other)
    for t in both:
        v, u = spots[t]
        mv.got(('oR', t))
        half = view(out_ref, t, v, step(u, -1), upper)
        mv.send(('o2R', t), half, half, at(t, v, step(u, 1)))
        mv.got(('oL', t))
        half = view(out_ref, t, v, step(u, 1), lower)
        mv.send(('o2L', t), half, half, at(t, v, step(u, -1)))
    offsets = (0, -1, 1, 2)
    for g in (1, 2, 3):
        for t in both:
            v, u = spots[t]
            if g == 3:
                mv.got(('o2R', t))
                mv.got(('o2L', t))
            piece = view(out_ref, t, v, step(u, offsets[g]))
            mv.send(('pR', t, g), piece, piece, at(t, step(v, 1), u))
            mv.send(('pL', t, g), piece, piece, at(t, step(v, -1), u))
            mv.send(('s', t, 0, g), piece, piece, other)
    for g in range(4):
        for t in both:
            v, u = spots[t]
            mv.got(('pR', t, g))
            piece = view(out_ref, t, step(v, -1), step(u, offsets[g]))
            if g in (0, 2):
                mv.send(('z', t, g), piece, piece, at(t, step(v, 1), u))
            mv.send(('s', t, 1, g), piece, piece, other)
            mv.got(('pL', t, g))
            piece = view(out_ref, t, step(v, 1), step(u, offsets[g]))
            if g in (1, 3):
                mv.send(('z', t, g), piece, piece, at(t, step(v, -1), u))
            mv.send(('s', t, 2, g), piece, piece, other)
    for g in range(4):
        for t in both:
            v, u = spots[t]
            mv.got(('z', t, g))
            piece = view(out_ref, t, step(v, 2), step(u, offsets[g]))
            mv.send(('s', t, 3, g), piece, piece, other)
    for t in both:
        mv.done(('own', t))
        for i in range(4):
            for g in range(4):
                mv.got(('s', t, i, g))
    mv.finish()


ANY = pl.BlockSpec(memory_space=pl.ANY)
VMEM = pl.BlockSpec(memory_space=pltpu.VMEM)


def sems(n):
    return [pltpu.SemaphoreType.DMA((n,)), pltpu.SemaphoreType.DMA((n,))]


def project_queries(side, hidden, w_query, w_out):
    rows, dim = hidden.shape[3:]
    half = w_query.shape[1]
    w_rows, width = w_out.shape[0], w_out.shape[1] // (2 * side)
    bf16 = jnp.bfloat16
    tile = jax.ShapeDtypeStruct((side, CORES, w_rows, width), bf16)
    return pl.pallas_call(
        functools.partial(query_kernel, side),
        out_shape=[jax.ShapeDtypeStruct((side, side, rows, CORES * half), bf16), tile, tile],
        in_specs=[ANY] * 3,
        out_specs=[ANY] * 3,
        scratch_shapes=[
            pltpu.VMEM((CORES, dim, half), bf16),
            pltpu.VMEM((side, side, rows, dim), bf16),
            pltpu.VMEM((side, side, rows, CORES * half), bf16),
            pltpu.VMEM((side * rows, half), jnp.float32),
            pltpu.VMEM((2, 2, w_rows // 2, width), bf16),
            pltpu.VMEM((2, w_rows, width), bf16),
        ] + sems(64),
        compiler_params=pltpu.CompilerParams(collective_id=0, has_side_effects=True, vmem_limit_bytes=60 << 20),
        name='project_queries',
    )(hidden, w_query, w_out)


def project_context(side, context, w_a, w_b, hidden):
    rows, depth = context.shape[2:]
    width = w_a.shape[-1]
    bf16, f32 = jnp.bfloat16, jnp.float32
    return pl.pallas_call(
        functools.partial(output_kernel, side),
        out_shape=jax.ShapeDtypeStruct(hidden.shape, bf16),
        in_specs=[VMEM, ANY, ANY, ANY],
        out_specs=ANY,
        scratch_shapes=[
            pltpu.VMEM((2, side, side, side, rows, depth), bf16),
            pltpu.VMEM((2,) + w_a.shape, bf16),
            pltpu.VMEM((2, side, rows, width), bf16),
            pltpu.VMEM((2, side, rows, width), f32),
            pltpu.VMEM((2, 4, side, rows, width), bf16),
            pltpu.VMEM((2, 2, side // 2, rows, width), bf16),
            pltpu.VMEM((2, 2, side, rows, width), bf16),
            pltpu.VMEM((2, side, rows, width), bf16),
        ] + sems(128),
        compiler_params=pltpu.CompilerParams(collective_id=1, has_side_effects=True, vmem_limit_bytes=60 << 20),
        name='project_context',
    )(context, w_a, w_b, hidden)


def solution(mesh):
    side = math.isqrt(mesh.shape['model'] // CORES)

    def group_step(hidden, w_query, w_key, w_value, w_out, key_cache, value_cache, lengths):
        n_rows, dim = hidden.shape
        local_rows = key_cache.shape[0]
        head_dim = key_cache.shape[2]
        chip_cols = CORES * w_query.shape[1]
        n_heads = side * side * chip_cols // head_dim
        row_start = lax.axis_index('model') * local_rows
        hidden_tiles = hidden.reshape(side, side, CORES, local_rows, dim)
        query, w_a, w_b = project_queries(side, hidden_tiles, w_query, w_out)
        query = query.reshape(side * side, local_rows, chip_cols // head_dim, head_dim).transpose(1, 0, 2, 3).reshape(local_rows, n_heads, head_dim)
        hidden_local = lax.dynamic_slice_in_dim(hidden, row_start, local_rows, 0)
        len_local = lax.dynamic_slice_in_dim(lengths, row_start, local_rows, 0)
        key_new = jnp.dot(hidden_local, w_key, preferred_element_type=jnp.float32).astype(jnp.bfloat16)
        value_new = jnp.dot(hidden_local, w_value, preferred_element_type=jnp.float32).astype(jnp.bfloat16)
        key_upd, value_upd, context = attend(len_local, query, key_new, value_new, key_cache, value_cache)
        context = context.reshape(local_rows, side * side, chip_cols // head_dim, head_dim).transpose(1, 0, 2, 3).reshape(side, side, local_rows, chip_cols)
        hidden_out = project_context(side, context, w_a, w_b, hidden_tiles)
        return hidden_out.reshape(n_rows, dim), key_upd, value_upd

    row_spec = P('replica', None)
    cache_spec = P(('replica', 'model'), None, None)
    return jax.shard_map(group_step, mesh=mesh, in_specs=(row_spec, P(None, 'model'), P(None, None), P(None, None), P('model', None), cache_spec, cache_spec, P('replica')), out_specs=(row_spec, cache_spec, cache_spec), check_vma=False)
```

```python
import functools
import math
import jax
import jax.numpy as jnp
from jax import lax
from jax.experimental import pallas as pl
from jax.experimental.pallas import tpu as pltpu
from jax.sharding import PartitionSpec as P

CHUNK = 16


def attend_rows(query, keys, values, row_lens, score_scale):
    seq_len = keys[0].shape[0]
    positions = lax.broadcasted_iota(jnp.int32, (1, seq_len), 1)
    scores = [
        lax.dot_general(q, k, (((1,), (1,)), ((), ())), preferred_element_type=jnp.float32) + jnp.where(positions <= n, 0.0, -jnp.inf)
        for q, k, n in zip(query, keys, row_lens)
    ]
    weights = [jnp.exp2((s - jnp.max(s, axis=1, keepdims=True)) * (score_scale * math.log2(math.e))) for s in scores]
    sums = [jnp.sum(e, axis=1, keepdims=True) for e in weights]
    return [(jnp.dot(e.astype(jnp.bfloat16), v, preferred_element_type=jnp.float32) / t).astype(jnp.bfloat16) for e, v, t in zip(weights, values, sums)]


def attend_kernel(len_ref, q_hbm, new_ref, k_hbm, v_hbm, ko_hbm, vo_hbm, ctx_ref, q_ref, k_ref, v_ref, q_sem, in_sems, out_sems):
    n, seq_len, head_dim = k_ref.shape
    tile = math.gcd(seq_len, 16)
    first = lax.axis_index('model') * n

    def loads(i):
        part = pl.ds(i * CHUNK, CHUNK)
        return [pltpu.make_async_copy(src.at[part], dst.at[part], in_sems.at[j, i]) for j, (src, dst) in enumerate(((k_hbm, k_ref), (v_hbm, v_ref)))]

    def stores(i):
        part = pl.ds(i * CHUNK, CHUNK)
        return [pltpu.make_async_copy(src.at[part], dst.at[part], out_sems.at[j, i]) for j, (src, dst) in enumerate(((k_ref, ko_hbm), (v_ref, vo_hbm)))]

    q_copy = pltpu.make_async_copy(q_hbm, q_ref, q_sem)
    q_copy.start()
    for i in range(n // CHUNK):
        for copy in loads(i):
            copy.start()
    q_copy.wait()

    @pl.loop(0, n // CHUNK)
    def _(i):
        for copy in loads(i):
            copy.wait()
        rows = [i * CHUNK + r for r in range(CHUNK)]
        lens = [len_ref[first + r] for r in rows]
        for r, row_len in zip(rows, lens):
            base = pl.multiple_of((row_len // tile) * tile, tile)
            pick = lax.broadcasted_iota(jnp.int32, (tile, head_dim), 0) == row_len - base
            for j, ref in enumerate((k_ref, v_ref)):
                new = jnp.broadcast_to(new_ref[j, pl.ds(r, 1), :], (tile, head_dim))
                old = ref[r, pl.ds(base, tile), :].astype(jnp.float32)
                ref[r, pl.ds(base, tile), :] = jnp.where(pick, new, old).astype(jnp.bfloat16)
        out = attend_rows([q_ref[r] for r in rows], [k_ref[r] for r in rows], [v_ref[r] for r in rows], lens, head_dim ** -0.5)
        for r, ctx in zip(rows, out):
            ctx_ref[r] = ctx
        for copy in stores(i):
            copy.start()

    @pl.loop(0, n // CHUNK)
    def _(i):
        for copy in stores(i):
            copy.wait()


def attend(lens, query, new, key_cache, value_cache):
    n, seq_len, head_dim = key_cache.shape
    n_heads = query.shape[1]
    return pl.pallas_call(
        attend_kernel,
        in_specs=[pl.BlockSpec(memory_space=pltpu.SMEM), ANY, VMEM, ANY, ANY],
        out_specs=[ANY, ANY, VMEM],
        out_shape=[
            jax.ShapeDtypeStruct(key_cache.shape, key_cache.dtype),
            jax.ShapeDtypeStruct(value_cache.shape, value_cache.dtype),
            jax.ShapeDtypeStruct(query.shape, jnp.bfloat16),
        ],
        scratch_shapes=[
            pltpu.VMEM(query.shape, jnp.bfloat16),
            pltpu.VMEM(key_cache.shape, jnp.bfloat16),
            pltpu.VMEM(value_cache.shape, jnp.bfloat16),
            pltpu.SemaphoreType.DMA(()),
            pltpu.SemaphoreType.DMA((2, n // CHUNK)),
            pltpu.SemaphoreType.DMA((2, n // CHUNK)),
        ],
        compiler_params=pltpu.CompilerParams(vmem_limit_bytes=63 << 20),
        cost_estimate=pl.CostEstimate(flops=4 * n * n_heads * seq_len * head_dim, bytes_accessed=8 * n * seq_len * head_dim, transcendentals=0),
        name='attend',
    )(lens, query, new, key_cache, value_cache)


ANY = pl.BlockSpec(memory_space=pl.ANY)
VMEM = pl.BlockSpec(memory_space=pltpu.VMEM)


MESH = pl.DeviceIdType.MESH
CORES = 2


class Moves:
    def __init__(self, send_sems, recv_sems):
        self.send_sems, self.recv_sems = send_sems, recv_sems
        self.count, self.copies, self.unsent = 0, {}, []

    def send(self, key, src, dst, device):
        copy = pltpu.make_async_remote_copy(src_ref=src, dst_ref=dst, send_sem=self.send_sems.at[self.count], recv_sem=self.recv_sems.at[self.count], device_id={'model': device}, device_id_type=MESH)
        copy.start()
        self.count += 1
        self.copies[key] = copy
        self.unsent.append(copy)

    def local(self, key, src, dst):
        copy = pltpu.make_async_copy(src, dst, self.send_sems.at[self.count])
        copy.start()
        self.count += 1
        self.copies[key] = copy

    def got(self, key):
        self.copies.pop(key).wait_recv()

    def done(self, key):
        self.copies.pop(key).wait()

    def finish(self):
        for copy in self.unsent:
            copy.wait_send()


def place(side):
    me = lax.axis_index('model')
    return me // (CORES * side), lax.rem(me // CORES, side), lax.rem(me, CORES)


def greet(devices):
    barrier = pltpu.get_barrier_semaphore()
    for device in devices:
        pl.semaphore_signal(barrier, inc=1, device_id={'model': device}, device_id_type=MESH)
    pl.semaphore_wait(barrier, len(devices))


def columns(start, width):
    return pl.ds(pl.multiple_of(start * width, width), width)


def query_kernel(side, hid_ref, wq_ref, wo_ref, wk_ref, wv_ref, q_ref, wa_ref, wb_ref, new_ref, wq_all, hid, q_buf, acc, w_new, own_w, load_sems, send_sems, recv_sems):
    y, x, c = place(side)
    rows, dim = hid_ref.shape[3:]
    half = wq_ref.shape[1]
    w_rows = wo_ref.shape[0]
    width = wo_ref.shape[1] // (2 * side)
    w_refs = (wa_ref, wb_ref)
    step = lambda a, d: lax.rem(a + d + side, side)
    dev = lambda yy, xx: (yy * side + xx) * CORES + c
    other = (y * side + x) * CORES + 1 - c
    peers = [(dy, dx) for dy in range(side) for dx in range(side) if dy or dx]
    mv = Moves(send_sems, recv_sems)
    order = list(range(1, side)) + [0]
    depth, pair = min(2048, dim), side // 2

    def loads(k):
        part = columns(k, depth)
        pairs = [(wq_ref.at[part], wq_all.at[c, part])] + [(hid_ref.at[step(y, dy), :, c, :, part], hid.at[i, :, :, part]) for i, dy in enumerate(order)]
        return [pltpu.make_async_copy(src, dst, load_sems.at[j, k]) for j, (src, dst) in enumerate(pairs)]

    for k in range(dim // depth):
        for copy in loads(k):
            copy.start()
    greet([dev(step(y, dy), step(x, dx)) for dy, dx in peers] + [other])
    mv.send('wq', wq_ref, wq_all.at[c], other)
    along = ((x, lambda u: dev(y, u)), (y, lambda u: dev(u, x)))
    wcols = lambda t, u: columns(t * side + u, width)
    for t, (u, at) in enumerate(along):
        mv.send(('w', t, 2), wo_ref.at[:, wcols(t, step(u, 2))], w_refs[t].at[u, c], at(step(u, 2)))
        for d in (1, 3):
            mv.send(('w', t, d), wo_ref.at[:, wcols(t, step(u, d))], w_refs[t].at[u, c], at(step(u, d)))
        mv.local(('w_own', t), wo_ref.at[:, wcols(t, u)], own_w.at[t])
    for j, ref in enumerate((wk_ref, wv_ref)):
        mv.local(('w_new', j), ref, w_new.at[j])

    def gain(h, core, part):
        acc[h] += jnp.dot(hid[pl.ds(h * pair, pair), :, :, part].reshape(pair * side * rows, depth), wq_all[core, part, :], preferred_element_type=jnp.float32)

    def store(h, core):
        q_buf[pl.ds(h * pair, pair), :, :, columns(core, half)] = acc[h].astype(jnp.bfloat16).reshape(pair, side, rows, half)
        acc[h] = jnp.zeros_like(acc[h])

    acc[...] = jnp.zeros_like(acc)

    @pl.loop(0, dim // depth)
    def _(k):
        for copy in loads(k):
            copy.wait()
        for h in range(2):
            gain(h, c, columns(k, depth))

    for h in range(2):
        store(h, c)

    def project(h):
        @pl.loop(0, dim // depth)
        def _(k):
            gain(h, 1 - c, columns(k, depth))

        store(h, 1 - c)

    for t, (u, at) in enumerate(along):
        mv.done(('w_own', t))
        mv.local(('w_put', t), own_w.at[t], w_refs[t].at[u, c])
        mv.send(('wS', t, 0), own_w.at[t], w_refs[t].at[u, c], other)
    mv.got('wq')
    for i, dy in enumerate(order):
        if i % pair == 0:
            project(i // pair)
        for dx in [d for d in (2, 1, 3, 0)][:side]:
            if dy or dx:
                mv.send(('q', dy, dx), q_buf.at[i, step(x, dx)], q_ref.at[y, x], dev(step(y, dy), step(x, dx)))
            else:
                mv.local('q_own', q_buf.at[i, x], q_ref.at[y, x])
    for j in range(2):
        mv.done(('w_new', j))
        new = jnp.zeros((rows, w_new.shape[2]), jnp.float32)
        for k in range(0, dim, depth):
            new += jnp.dot(hid[side - 1, x, :, k:k + depth], w_new[j, k:k + depth, :], preferred_element_type=jnp.float32)
        new_ref[j] = new.astype(jnp.bfloat16).astype(jnp.float32)
    for d in (2, 1, 3):
        for t, (u, at) in enumerate(along):
            mv.got(('w', t, d))
            tile = w_refs[t].at[step(u, -d), c]
            mv.send(('wS', t, d), tile, tile, other)
    for dy, dx in peers:
        mv.got(('q', dy, dx))
    mv.done('q_own')
    for t in range(2):
        mv.done(('w_put', t))
        for d in range(side):
            mv.got(('wS', t, d))
    mv.finish()


def output_kernel(side, ctx_ref, wa_ref, wb_ref, hid_ref, out_ref, held, w_buf, acc, keep, part, first, second, final, send_sems, recv_sems):
    y, x, c = place(side)
    rows, depth = ctx_ref.shape[2:]
    width = w_buf.shape[-1]
    step = lambda a, d: lax.rem(a + d + side, side)
    dev = lambda yy, xx: (yy * side + xx) * CORES + c
    other = (y * side + x) * CORES + 1 - c
    spots = ((y, x), (x, y))
    at = lambda t, v, u: dev(v, u) if t == 0 else dev(u, v)
    ctx_of = lambda t, v: ctx_ref.at[v] if t == 0 else ctx_ref.at[:, v]
    greet([dev(y, step(x, d)) for d in range(1, side)] + [dev(step(y, d), x) for d in range(1, side)] + [other])
    mv = Moves(send_sems, recv_sems)
    both = range(2)

    def view(ref, t, v, g, us=None):
        us = slice(None) if us is None else us
        cols = columns(t * side + g, width)
        return ref.at[v, us, c, :, cols] if t == 0 else ref.at[us, v, c, :, cols]

    for t in both:
        v, u = spots[t]
        mv.send(('a', t, 2), ctx_of(t, step(v, 2)), held.at[t, u, v], at(t, step(v, 2), u))
    for t in both:
        v, u = spots[t]
        for d in (1, 3):
            mv.send(('a', t, d), ctx_of(t, step(v, d)), held.at[t, u, v], at(t, step(v, d), u))
        mv.send(('gR', t, 0), ctx_of(t, v), held.at[t, u, v], at(t, v, step(u, 1)))
        mv.send(('gL', t, 0), ctx_of(t, v), held.at[t, u, v], at(t, v, step(u, -1)))
    for t in both:
        v, u = spots[t]
        mv.local(('w', t), (wa_ref, wb_ref)[t], w_buf.at[t])
        mv.local(('hid', t), view(hid_ref, t, v, u), final.at[t])

    def spread(t, p, tag):
        v, u = spots[t]
        slot = held.at[t, u, step(v, -p)]
        mv.send(('g' + tag, t, p), slot, slot, at(t, v, step(u, 1 if tag == 'R' else -1)))

    def forward(t, p, tag):
        v, u = spots[t]
        mv.got(('g' + tag, t, p))
        slot = held.at[t, step(u, -1 if tag == 'R' else 1), step(v, -p)]
        mv.send(('f', t, p), slot, slot, at(t, v, step(u, 1 if tag == 'R' else -1)))

    for t in both:
        mv.got(('a', t, 2))
        spread(t, 2, 'R')
        mv.got(('a', t, 1))
        spread(t, 1, 'L')
        spread(t, 2, 'L')
        spread(t, 1, 'R')
    for t in both:
        forward(t, 2, 'R')
        forward(t, 1, 'L')
        mv.got(('a', t, 3))
        spread(t, 3, 'R')
        spread(t, 3, 'L')
    for t in both:
        forward(t, 0, 'R')
    for t in both:
        mv.done(('w', t))

    def product(t, p):
        v, u = spots[t]
        total = None
        for k in range(side):
            pieces = []
            for d in range(side):
                if p == 0 and d == 0:
                    pieces.append(ctx_ref[v, k] if t == 0 else ctx_ref[k, v])
                else:
                    pieces.append(held[t, step(u, d), step(v, -p), k])
            one = jnp.dot(jnp.concatenate(pieces, axis=0), w_buf[t, k].reshape(depth, width), preferred_element_type=jnp.float32)
            total = one if total is None else total + one
        acc[t] = total.reshape(side, rows, width)

    upper, lower = pl.ds(0, side // 2), pl.ds(side // 2, side // 2)
    for t in both:
        v, u = spots[t]
        mv.got(('gL', t, 2))
        mv.got(('f', t, 2))
        product(t, 2)
        part[t, 2] = acc[t].astype(jnp.bfloat16)
        mv.send(('r1R', t), part.at[t, 2, upper], first.at[t, 0], at(t, step(v, 1), u))
        mv.send(('r1L', t), part.at[t, 2, lower], first.at[t, 1], at(t, step(v, -1), u))
    for t in both:
        forward(t, 3, 'L')
    sides = ((1, upper, lower, 'L', 1), (3, lower, upper, 'R', 0))
    for p, now, later, tag, d in sides:
        for t in both:
            v, u = spots[t]
            mv.got(('gR', t, p))
            mv.got(('f', t, p))
            product(t, p)
            part[t, p, now] = acc[t, now].astype(jnp.bfloat16)
            mv.send(('r2' + tag, t), part.at[t, p, now], second.at[t, d, now], at(t, step(v, -p), u))
            keep[t, d] = acc[t, later]
    for p, now, later, tag, d in sides:
        for t in both:
            v, u = spots[t]
            mv.got(('r1' + tag, t))
            part[t, p, later] = (keep[t, d] + first[t, d].astype(jnp.float32)).astype(jnp.bfloat16)
            mv.send(('r3' + tag, t), part.at[t, p, later], second.at[t, d, later], at(t, step(v, -p), u))
    for t in both:
        mv.got(('gL', t, 0))
        mv.got(('f', t, 0))
        product(t, 0)
    for t in both:
        v, u = spots[t]
        for tag in 'RL':
            mv.got(('r2' + tag, t))
            mv.got(('r3' + tag, t))
        mv.done(('hid', t))
        for d in range(side):
            us = step(u, d)
            y_sum = acc[t, d] + second[t, 0, d].astype(jnp.float32) + second[t, 1, d].astype(jnp.float32)
            final[t, us] = (final[t, us].astype(jnp.float32) + y_sum).astype(jnp.bfloat16)
        mine = view(out_ref, t, v, u)
        mv.send(('oR', t), final.at[t], mine, at(t, v, step(u, 1)))
        mv.send(('oL', t), final.at[t], mine, at(t, v, step(u, -1)))
        mv.send(('pR', t, 0), final.at[t], mine, at(t, step(v, 1), u))
        mv.send(('pL', t, 0), final.at[t], mine, at(t, step(v, -1), u))
        mv.local(('own', t), final.at[t], mine)
        mv.send(('s', t, 0, 0), final.at[t], mine, other)
    for t in both:
        v, u = spots[t]
        mv.got(('oR', t))
        half = view(out_ref, t, v, step(u, -1), upper)
        mv.send(('o2R', t), half, half, at(t, v, step(u, 1)))
        mv.got(('oL', t))
        half = view(out_ref, t, v, step(u, 1), lower)
        mv.send(('o2L', t), half, half, at(t, v, step(u, -1)))
    offsets = (0, -1, 1, 2)
    for g in (1, 2, 3):
        for t in both:
            v, u = spots[t]
            if g == 3:
                mv.got(('o2R', t))
                mv.got(('o2L', t))
            piece = view(out_ref, t, v, step(u, offsets[g]))
            mv.send(('pR', t, g), piece, piece, at(t, step(v, 1), u))
            mv.send(('pL', t, g), piece, piece, at(t, step(v, -1), u))
            mv.send(('s', t, 0, g), piece, piece, other)
    for g in range(4):
        for t in both:
            v, u = spots[t]
            mv.got(('pR', t, g))
            piece = view(out_ref, t, step(v, -1), step(u, offsets[g]))
            if g in (0, 2):
                mv.send(('z', t, g), piece, piece, at(t, step(v, 1), u))
            mv.send(('s', t, 1, g), piece, piece, other)
            mv.got(('pL', t, g))
            piece = view(out_ref, t, step(v, 1), step(u, offsets[g]))
            if g in (1, 3):
                mv.send(('z', t, g), piece, piece, at(t, step(v, -1), u))
            mv.send(('s', t, 2, g), piece, piece, other)
    for g in range(4):
        for t in both:
            v, u = spots[t]
            mv.got(('z', t, g))
            piece = view(out_ref, t, step(v, 2), step(u, offsets[g]))
            mv.send(('s', t, 3, g), piece, piece, other)
    for t in both:
        mv.done(('own', t))
        for i in range(4):
            for g in range(4):
                mv.got(('s', t, i, g))
    mv.finish()


def sems(n):
    return [pltpu.SemaphoreType.DMA((n,)), pltpu.SemaphoreType.DMA((n,))]


def project_queries(side, hidden, w_query, w_out, w_key, w_value):
    rows, dim = hidden.shape[3:]
    half = w_query.shape[1]
    w_rows, width = w_out.shape[0], w_out.shape[1] // (2 * side)
    bf16 = jnp.bfloat16
    tile = jax.ShapeDtypeStruct((side, CORES, w_rows, width), bf16)
    return pl.pallas_call(
        functools.partial(query_kernel, side),
        out_shape=[jax.ShapeDtypeStruct((side, side, rows, CORES * half), bf16), tile, tile, jax.ShapeDtypeStruct((2, rows, w_key.shape[1]), jnp.float32)],
        in_specs=[ANY] * 5,
        out_specs=[ANY] * 3 + [VMEM],
        scratch_shapes=[
            pltpu.VMEM((CORES, dim, half), bf16),
            pltpu.VMEM((side, side, rows, dim), bf16),
            pltpu.VMEM((side, side, rows, CORES * half), bf16),
            pltpu.VMEM((2, side // 2 * side * rows, half), jnp.float32),
            pltpu.VMEM((2,) + w_key.shape, bf16),
            pltpu.VMEM((2, w_rows, width), bf16),
            pltpu.SemaphoreType.DMA((1 + side, dim // min(2048, dim))),
        ] + sems(64),
        compiler_params=pltpu.CompilerParams(collective_id=0, has_side_effects=True, vmem_limit_bytes=63 << 20),
        name='project_queries',
    )(hidden, w_query, w_out, w_key, w_value)


def project_context(side, context, w_a, w_b, hidden):
    rows, depth = context.shape[2:]
    width = w_a.shape[-1]
    bf16, f32 = jnp.bfloat16, jnp.float32
    return pl.pallas_call(
        functools.partial(output_kernel, side),
        out_shape=pltpu.VMEM(hidden.shape, bf16),
        in_specs=[VMEM, ANY, ANY, ANY],
        out_specs=ANY,
        scratch_shapes=[
            pltpu.VMEM((2, side, side, side, rows, depth), bf16),
            pltpu.VMEM((2,) + w_a.shape, bf16),
            pltpu.VMEM((2, side, rows, width), f32),
            pltpu.VMEM((2, 2, side // 2, rows, width), f32),
            pltpu.VMEM((2, 4, side, rows, width), bf16),
            pltpu.VMEM((2, 2, side // 2, rows, width), bf16),
            pltpu.VMEM((2, 2, side, rows, width), bf16),
            pltpu.VMEM((2, side, rows, width), bf16),
        ] + sems(128),
        compiler_params=pltpu.CompilerParams(collective_id=1, has_side_effects=True, vmem_limit_bytes=30 << 20),
        name='project_context',
    )(context, w_a, w_b, hidden)


def put_kernel(src_ref, dst_ref, copy_sems):
    n = src_ref.shape[0] * src_ref.shape[1]
    side = src_ref.shape[1]
    copies = [pltpu.make_async_copy(src_ref.at[i // side, i % side], dst_ref.at[i // side, i % side], copy_sems.at[i]) for i in range(n)]
    for copy in copies:
        copy.start()
    for copy in copies:
        copy.wait()


def put(result):
    return pl.pallas_call(
        put_kernel,
        out_shape=jax.ShapeDtypeStruct(result.shape, result.dtype),
        in_specs=[ANY],
        out_specs=ANY,
        scratch_shapes=[pltpu.SemaphoreType.DMA((result.shape[0] * result.shape[1],))],
        compiler_params=pltpu.CompilerParams(vmem_limit_bytes=1 << 20),
        name='put',
    )(result)


def solution(mesh):
    side = math.isqrt(mesh.shape['model'] // CORES)

    def group_step(hidden, w_query, w_key, w_value, w_out, key_cache, value_cache, lengths):
        n_rows, dim = hidden.shape
        local_rows = key_cache.shape[0]
        head_dim = key_cache.shape[2]
        chip_cols = CORES * w_query.shape[1]
        n_heads = side * side * chip_cols // head_dim
        hidden_tiles = hidden.reshape(side, side, CORES, local_rows, dim)
        query, w_a, w_b, new = project_queries(side, hidden_tiles, w_query, w_out, w_key, w_value)
        query = query.reshape(side * side, local_rows, chip_cols // head_dim, head_dim).transpose(1, 0, 2, 3).reshape(local_rows, n_heads, head_dim)
        key_upd, value_upd, context = attend(lengths, query, new, key_cache, value_cache)
        context = context.reshape(local_rows, side * side, chip_cols // head_dim, head_dim).transpose(1, 0, 2, 3).reshape(side, side, local_rows, chip_cols)
        hidden_out = put(project_context(side, context, w_a, w_b, hidden_tiles))
        return hidden_out.reshape(n_rows, dim), key_upd, value_upd

    row_spec = P('replica', None)
    cache_spec = P(('replica', 'model'), None, None)
    return jax.shard_map(group_step, mesh=mesh, in_specs=(row_spec, P(None, 'model'), P(None, None), P(None, None), P('model', None), cache_spec, cache_spec, P('replica')), out_specs=(row_spec, cache_spec, cache_spec), check_vma=False)
```

```python
import functools
import math
import jax
import jax.numpy as jnp
from jax import lax
from jax.experimental import pallas as pl
from jax.experimental.pallas import tpu as pltpu
from jax.sharding import PartitionSpec as P

CHUNK = 16


def attend_rows(query, keys, values, new_keys, new_values, row_lens, score_scale):
    positions = lax.broadcasted_iota(jnp.int32, (1, keys[0].shape[0]), 1)
    factor = score_scale * math.log2(math.e)
    old = [
        lax.dot_general(q.astype(jnp.bfloat16), k, (((1,), (1,)), ((), ())), preferred_element_type=jnp.float32) + jnp.where(positions < n, 0.0, -jnp.inf)
        for q, k, n in zip(query, keys, row_lens)
    ]
    own = [jnp.sum(q * k, axis=1, keepdims=True) for q, k in zip(query, new_keys)]
    tops = [jnp.maximum(jnp.max(s, axis=1, keepdims=True), o) for s, o in zip(old, own)]
    old = [jnp.exp2((s - t) * factor) for s, t in zip(old, tops)]
    own = [jnp.exp2((o - t) * factor) for o, t in zip(own, tops)]
    sums = [jnp.sum(s, axis=1, keepdims=True) + o for s, o in zip(old, own)]
    mixed = [jnp.dot(s.astype(jnp.bfloat16), v, preferred_element_type=jnp.float32) for s, v in zip(old, values)]
    return [(m + o.astype(jnp.bfloat16).astype(jnp.float32) * v) / t for m, o, v, t in zip(mixed, own, new_values, sums)]


def update_kernel(len_ref, new_ref, k_hbm, v_hbm, ko_hbm, vo_hbm, k_ref, v_ref, in_sems, out_sems):
    n, seq_len, head_dim = k_ref.shape
    tile = math.gcd(seq_len, 16)
    first = lax.axis_index('model') * n

    def loads(i):
        part = pl.ds(i * CHUNK, CHUNK)
        return [pltpu.make_async_copy(src.at[part], dst.at[part], in_sems.at[j, i]) for j, (src, dst) in enumerate(((k_hbm, k_ref), (v_hbm, v_ref)))]

    def stores(i):
        part = pl.ds(i * CHUNK, CHUNK)
        return [pltpu.make_async_copy(src.at[part], dst.at[part], out_sems.at[j, i]) for j, (src, dst) in enumerate(((k_ref, ko_hbm), (v_ref, vo_hbm)))]

    for i in range(n // CHUNK):
        for copy in loads(i):
            copy.start()

    @pl.loop(0, n // CHUNK)
    def _(i):
        for copy in loads(i):
            copy.wait()
        for r in range(CHUNK):
            r = i * CHUNK + r
            row_len = len_ref[first + r]
            base = pl.multiple_of((row_len // tile) * tile, tile)
            pick = lax.broadcasted_iota(jnp.int32, (tile, head_dim), 0) == row_len - base
            for j, ref in enumerate((k_ref, v_ref)):
                new = jnp.broadcast_to(new_ref[j, pl.ds(r, 1), :], (tile, head_dim))
                old = ref[r, pl.ds(base, tile), :].astype(jnp.float32)
                ref[r, pl.ds(base, tile), :] = jnp.where(pick, new, old).astype(jnp.bfloat16)
        for copy in stores(i):
            copy.start()

    @pl.loop(0, n // CHUNK)
    def _(i):
        for copy in stores(i):
            copy.wait()


def update(lens, new, key_cache, value_cache):
    n = key_cache.shape[0]
    return pl.pallas_call(
        update_kernel,
        in_specs=[pl.BlockSpec(memory_space=pltpu.SMEM), VMEM, ANY, ANY],
        out_specs=[ANY] * 2,
        out_shape=[jax.ShapeDtypeStruct(x.shape, x.dtype) for x in (key_cache, value_cache)],
        scratch_shapes=[
            pltpu.VMEM(key_cache.shape, jnp.bfloat16),
            pltpu.VMEM(value_cache.shape, jnp.bfloat16),
            pltpu.SemaphoreType.DMA((2, n // CHUNK)),
            pltpu.SemaphoreType.DMA((2, n // CHUNK)),
        ],
        compiler_params=pltpu.CompilerParams(vmem_limit_bytes=63 << 20),
        name='update',
    )(lens, new, key_cache, value_cache)


ANY = pl.BlockSpec(memory_space=pl.ANY)
VMEM = pl.BlockSpec(memory_space=pltpu.VMEM)


MESH = pl.DeviceIdType.MESH
CORES = 2
EARLY = (2,)


class Moves:
    def __init__(self, send_sems, recv_sems):
        self.send_sems, self.recv_sems = send_sems, recv_sems
        self.count, self.copies, self.unsent = 0, {}, []

    def send(self, key, src, dst, device):
        copy = pltpu.make_async_remote_copy(src_ref=src, dst_ref=dst, send_sem=self.send_sems.at[self.count], recv_sem=self.recv_sems.at[self.count], device_id={'model': device}, device_id_type=MESH)
        copy.start()
        self.count += 1
        self.copies[key] = copy
        self.unsent.append(copy)

    def local(self, key, src, dst):
        copy = pltpu.make_async_copy(src, dst, self.send_sems.at[self.count])
        copy.start()
        self.count += 1
        self.copies[key] = copy

    def got(self, key):
        self.copies.pop(key).wait_recv()

    def done(self, key):
        self.copies.pop(key).wait()

    def finish(self):
        for copy in self.unsent:
            copy.wait_send()


def place(side):
    me = lax.axis_index('model')
    return me // (CORES * side), lax.rem(me // CORES, side), lax.rem(me, CORES)


def greet(devices):
    barrier = pltpu.get_barrier_semaphore()
    for device in devices:
        pl.semaphore_signal(barrier, inc=1, device_id={'model': device}, device_id_type=MESH)
    pl.semaphore_wait(barrier, len(devices))


def columns(start, width):
    return pl.ds(pl.multiple_of(start * width, width), width)


def attend_kernel(side, len_ref, hid_ref, wq_ref, wo_ref, wk_ref, wv_ref, k_hbm, v_hbm, wa_ref, wb_ref, new_ref, ctx_ref, wq_all, hid, q_buf, q_got, acc, w_new, own_w, k_ref, v_ref, q_rows, ctx_rows, load_sems, send_sems, recv_sems):
    y, x, c = place(side)
    rows, dim = hid_ref.shape[3:]
    half = wq_ref.shape[1]
    w_rows = wo_ref.shape[0]
    width = wo_ref.shape[1] // (2 * side)
    w_refs = (wa_ref, wb_ref)
    step = lambda a, d: lax.rem(a + d + side, side)
    dev = lambda yy, xx: (yy * side + xx) * CORES + c
    other = (y * side + x) * CORES + 1 - c
    peers = [(dy, dx) for dy in range(side) for dx in range(side) if dy or dx]
    mv = Moves(send_sems, recv_sems)
    order = list(range(1, side)) + [0]
    depth, pair = min(2048, dim), side // 2

    def loads(k):
        part = columns(k, depth)
        pairs = [(wq_ref.at[part], wq_all.at[c, part])] + [(hid_ref.at[step(y, dy), :, c, :, part], hid.at[i, :, :, part]) for i, dy in enumerate(order)]
        return [pltpu.make_async_copy(src, dst, load_sems.at[j, k]) for j, (src, dst) in enumerate(pairs)]

    for k in range(dim // depth):
        for copy in loads(k):
            copy.start()
    greet([dev(step(y, dy), step(x, dx)) for dy, dx in peers] + [other])
    mv.send('wq', wq_ref, wq_all.at[c], other)
    along = ((x, lambda u: dev(y, u)), (y, lambda u: dev(u, x)))
    wcols = lambda t, u: columns(t * side + u, width)
    for t, (u, at) in enumerate(along):
        for d in EARLY:
            mv.send(('w', t, d), wo_ref.at[:, wcols(t, step(u, d))], w_refs[t].at[u], at(step(u, d)))
        mv.local(('w_own', t), wo_ref.at[:, wcols(t, u)], own_w.at[t])
    for j, ref in enumerate((wk_ref, wv_ref)):
        mv.local(('w_new', j), ref, w_new.at[j])
    for j, (src, dst) in enumerate(((k_hbm, k_ref), (v_hbm, v_ref))):
        mv.local(('cache', j), src, dst)

    def gain(h, core, part):
        acc[h] += jnp.dot(hid[pl.ds(h * pair, pair), :, :, part].reshape(pair * side * rows, depth), wq_all[core, part, :], preferred_element_type=jnp.float32)

    def store(h, core):
        q_buf[pl.ds(h * pair, pair), :, :, columns(core, half)] = acc[h].astype(jnp.bfloat16).reshape(pair, side, rows, half)
        acc[h] = jnp.zeros_like(acc[h])

    acc[...] = jnp.zeros_like(acc)

    @pl.loop(0, dim // depth)
    def _(k):
        for copy in loads(k):
            copy.wait()
        for h in range(2):
            gain(h, c, columns(k, depth))

    for h in range(2):
        store(h, c)

    def project(h):
        @pl.loop(0, dim // depth)
        def _(k):
            gain(h, 1 - c, columns(k, depth))

        store(h, 1 - c)

    for t, (u, at) in enumerate(along):
        mv.done(('w_own', t))
        mv.local(('w_put', t), own_w.at[t], w_refs[t].at[u])
    mv.got('wq')
    for i, dy in enumerate(order):
        if i % pair == 0:
            project(i // pair)
        for dx in [d for d in (2, 1, 3, 0)][:side]:
            if dy or dx:
                mv.send(('q', dy, dx), q_buf.at[i, step(x, dx)], q_got.at[y, x], dev(step(y, dy), step(x, dx)))
            else:
                q_got[y, x] = q_buf[i, x]
    for t, (u, at) in enumerate(along):
        for d in range(1, side):
            if d not in EARLY:
                mv.send(('w', t, d), wo_ref.at[:, wcols(t, step(u, d))], w_refs[t].at[u], at(step(u, d)))
    for j in range(2):
        mv.done(('w_new', j))
        new = jnp.zeros((rows, w_new.shape[2]), jnp.float32)
        for k in range(0, dim, depth):
            new += jnp.dot(hid[side - 1, x, :, k:k + depth], w_new[j, k:k + depth, :], preferred_element_type=jnp.float32)
        new_ref[j] = new.astype(jnp.bfloat16).astype(jnp.float32)
        mv.done(('cache', j))
    for dy, dx in peers:
        mv.got(('q', dy, dx))

    chips, head_dim = side * side, k_ref.shape[2]
    chunk = min(CHUNK, rows)
    lanes = [slice(h * head_dim, (h + 1) * head_dim) for h in range(CORES * half // head_dim)]
    first = lax.axis_index('model') * rows

    @pl.loop(0, rows // chunk)
    def _(i):
        part = pl.ds(pl.multiple_of(i * chunk, chunk), chunk)
        for h, lane in enumerate(lanes):
            q_rows[h] = q_got[:, :, part, lane].astype(jnp.float32).reshape(chips * chunk, head_dim)
        some = [i * chunk + r for r in range(chunk)]
        query = []
        for r in range(chunk):
            query.append(jnp.concatenate([q_rows[h, pl.ds(r, chips, stride=chunk), :] for h in range(len(lanes))], axis=0))
        new_keys, new_values = ([new_ref[j, pl.ds(r, 1), :] for r in some] for j in range(2))
        out = attend_rows(query, [k_ref[r] for r in some], [v_ref[r] for r in some], new_keys, new_values, [len_ref[first + r] for r in some], head_dim ** -0.5)
        for r in range(chunk):
            for h in range(len(lanes)):
                ctx_rows[h, pl.ds(r, chips, stride=chunk), :] = out[r][h * chips:(h + 1) * chips]
        for h, lane in enumerate(lanes):
            ctx_ref[:, :, part, lane] = ctx_rows[h].astype(jnp.bfloat16).reshape(side, side, chunk, head_dim)

    for t in range(2):
        mv.done(('w_put', t))
        for d in range(1, side):
            mv.got(('w', t, d))
    mv.finish()


def output_kernel(side, ctx_ref, wa_ref, wb_ref, hid_ref, out_ref, held, w_buf, acc, keep, part, first, second, final, send_sems, recv_sems):
    y, x, c = place(side)
    rows, depth = ctx_ref.shape[2:]
    width = w_buf.shape[-1]
    step = lambda a, d: lax.rem(a + d + side, side)
    dev = lambda yy, xx: (yy * side + xx) * CORES + c
    other = (y * side + x) * CORES + 1 - c
    spots = ((y, x), (x, y))
    at = lambda t, v, u: dev(v, u) if t == 0 else dev(u, v)
    ctx_of = lambda t, v: ctx_ref.at[v] if t == 0 else ctx_ref.at[:, v]
    greet([dev(y, step(x, d)) for d in range(1, side)] + [dev(step(y, d), x) for d in range(1, side)] + [other])
    mv = Moves(send_sems, recv_sems)
    both = range(2)

    def view(ref, t, v, g, us=None):
        us = slice(None) if us is None else us
        cols = columns(t * side + g, width)
        return ref.at[v, us, c, :, cols] if t == 0 else ref.at[us, v, c, :, cols]

    for t in both:
        v, u = spots[t]
        mv.send(('a', t, 2), ctx_of(t, step(v, 2)), held.at[t, u, v], at(t, step(v, 2), u))
    for t in both:
        v, u = spots[t]
        for d in (1, 3):
            mv.send(('a', t, d), ctx_of(t, step(v, d)), held.at[t, u, v], at(t, step(v, d), u))
        mv.send(('gR', t, 0), ctx_of(t, v), held.at[t, u, v], at(t, v, step(u, 1)))
        mv.send(('gL', t, 0), ctx_of(t, v), held.at[t, u, v], at(t, v, step(u, -1)))
    for t in both:
        v, u = spots[t]
        mv.local(('w', t), (wa_ref, wb_ref)[t], w_buf.at[t, :, c])
        mv.send(('wS', t), (wa_ref, wb_ref)[t], w_buf.at[t, :, c], other)
        mv.local(('hid', t), view(hid_ref, t, v, u), final.at[t])

    def spread(t, p, tag):
        v, u = spots[t]
        slot = held.at[t, u, step(v, -p)]
        mv.send(('g' + tag, t, p), slot, slot, at(t, v, step(u, 1 if tag == 'R' else -1)))

    def forward(t, p, tag):
        v, u = spots[t]
        mv.got(('g' + tag, t, p))
        slot = held.at[t, step(u, -1 if tag == 'R' else 1), step(v, -p)]
        mv.send(('f', t, p), slot, slot, at(t, v, step(u, 1 if tag == 'R' else -1)))

    for t in both:
        mv.got(('a', t, 2))
        spread(t, 2, 'R')
        mv.got(('a', t, 1))
        spread(t, 1, 'L')
        spread(t, 2, 'L')
        spread(t, 1, 'R')
    for t in both:
        forward(t, 2, 'R')
        forward(t, 1, 'L')
        mv.got(('a', t, 3))
        spread(t, 3, 'R')
        spread(t, 3, 'L')
    for t in both:
        forward(t, 0, 'R')
    for t in both:
        mv.done(('w', t))
        mv.got(('wS', t))

    def product(t, p):
        v, u = spots[t]
        total = None
        for k in range(side):
            pieces = []
            for d in range(side):
                if p == 0 and d == 0:
                    pieces.append(ctx_ref[v, k] if t == 0 else ctx_ref[k, v])
                else:
                    pieces.append(held[t, step(u, d), step(v, -p), k])
            one = jnp.dot(jnp.concatenate(pieces, axis=0), w_buf[t, k].reshape(depth, width), preferred_element_type=jnp.float32)
            total = one if total is None else total + one
        acc[t] = total.reshape(side, rows, width)

    upper, lower = pl.ds(0, side // 2), pl.ds(side // 2, side // 2)
    for t in both:
        v, u = spots[t]
        mv.got(('gL', t, 2))
        mv.got(('f', t, 2))
        product(t, 2)
        part[t, 2] = acc[t].astype(jnp.bfloat16)
        mv.send(('r1R', t), part.at[t, 2, upper], first.at[t, 0], at(t, step(v, 1), u))
        mv.send(('r1L', t), part.at[t, 2, lower], first.at[t, 1], at(t, step(v, -1), u))
    for t in both:
        forward(t, 3, 'L')
    sides = ((1, upper, lower, 'L', 1), (3, lower, upper, 'R', 0))
    for p, now, later, tag, d in sides:
        for t in both:
            v, u = spots[t]
            mv.got(('gR', t, p))
            mv.got(('f', t, p))
            product(t, p)
            part[t, p, now] = acc[t, now].astype(jnp.bfloat16)
            mv.send(('r2' + tag, t), part.at[t, p, now], second.at[t, d, now], at(t, step(v, -p), u))
            keep[t, d] = acc[t, later]
    for p, now, later, tag, d in sides:
        for t in both:
            v, u = spots[t]
            mv.got(('r1' + tag, t))
            part[t, p, later] = (keep[t, d] + first[t, d].astype(jnp.float32)).astype(jnp.bfloat16)
            mv.send(('r3' + tag, t), part.at[t, p, later], second.at[t, d, later], at(t, step(v, -p), u))
    for t in both:
        mv.got(('gL', t, 0))
        mv.got(('f', t, 0))
        product(t, 0)
    for t in both:
        v, u = spots[t]
        for tag in 'RL':
            mv.got(('r2' + tag, t))
            mv.got(('r3' + tag, t))
        mv.done(('hid', t))
        for d in range(side):
            us = step(u, d)
            y_sum = acc[t, d] + second[t, 0, d].astype(jnp.float32) + second[t, 1, d].astype(jnp.float32)
            final[t, us] = (final[t, us].astype(jnp.float32) + y_sum).astype(jnp.bfloat16)
        mine = view(out_ref, t, v, u)
        mv.send(('oR', t), final.at[t], mine, at(t, v, step(u, 1)))
        mv.send(('oL', t), final.at[t], mine, at(t, v, step(u, -1)))
        mv.send(('pR', t, 0), final.at[t], mine, at(t, step(v, 1), u))
        mv.send(('pL', t, 0), final.at[t], mine, at(t, step(v, -1), u))
        mv.local(('own', t), final.at[t], mine)
        mv.send(('s', t, 0, 0), final.at[t], mine, other)
    for t in both:
        v, u = spots[t]
        mv.got(('oR', t))
        half = view(out_ref, t, v, step(u, -1), upper)
        mv.send(('o2R', t), half, half, at(t, v, step(u, 1)))
        mv.got(('oL', t))
        half = view(out_ref, t, v, step(u, 1), lower)
        mv.send(('o2L', t), half, half, at(t, v, step(u, -1)))
    offsets = (0, -1, 1, 2)
    for g in (1, 2, 3):
        for t in both:
            v, u = spots[t]
            if g == 3:
                mv.got(('o2R', t))
                mv.got(('o2L', t))
            piece = view(out_ref, t, v, step(u, offsets[g]))
            mv.send(('pR', t, g), piece, piece, at(t, step(v, 1), u))
            mv.send(('pL', t, g), piece, piece, at(t, step(v, -1), u))
            mv.send(('s', t, 0, g), piece, piece, other)
    for g in range(4):
        for t in both:
            v, u = spots[t]
            mv.got(('pR', t, g))
            piece = view(out_ref, t, step(v, -1), step(u, offsets[g]))
            if g in (0, 2):
                mv.send(('z', t, g), piece, piece, at(t, step(v, 1), u))
            mv.send(('s', t, 1, g), piece, piece, other)
            mv.got(('pL', t, g))
            piece = view(out_ref, t, step(v, 1), step(u, offsets[g]))
            if g in (1, 3):
                mv.send(('z', t, g), piece, piece, at(t, step(v, -1), u))
            mv.send(('s', t, 2, g), piece, piece, other)
    for g in range(4):
        for t in both:
            v, u = spots[t]
            mv.got(('z', t, g))
            piece = view(out_ref, t, step(v, 2), step(u, offsets[g]))
            mv.send(('s', t, 3, g), piece, piece, other)
    for t in both:
        mv.done(('own', t))
        for i in range(4):
            for g in range(4):
                mv.got(('s', t, i, g))
    mv.finish()


def sems(n):
    return [pltpu.SemaphoreType.DMA((n,)), pltpu.SemaphoreType.DMA((n,))]


def attend(side, lens, hidden, w_query, w_out, w_key, w_value, key_cache, value_cache):
    rows, dim = hidden.shape[3:]
    half = w_query.shape[1]
    w_rows, width = w_out.shape[0], w_out.shape[1] // (2 * side)
    bf16, f32 = jnp.bfloat16, jnp.float32
    tile = jax.ShapeDtypeStruct((side, w_rows, width), bf16)
    wide = (side, side, rows, CORES * half)
    depth = min(2048, dim)
    return pl.pallas_call(
        functools.partial(attend_kernel, side),
        out_shape=[tile, tile, jax.ShapeDtypeStruct((2, rows, w_key.shape[1]), f32), jax.ShapeDtypeStruct(wide, bf16)],
        in_specs=[pl.BlockSpec(memory_space=pltpu.SMEM)] + [ANY] * 7,
        out_specs=[ANY, ANY, VMEM, VMEM],
        scratch_shapes=[
            pltpu.VMEM((CORES, dim, half), bf16),
            pltpu.VMEM((side, side, rows, dim), bf16),
            pltpu.VMEM(wide, bf16),
            pltpu.VMEM(wide, bf16),
            pltpu.VMEM((2, side // 2 * side * rows, half), f32),
            pltpu.VMEM((2,) + w_key.shape, bf16),
            pltpu.VMEM((2, w_rows, width), bf16),
            pltpu.VMEM(key_cache.shape, bf16),
            pltpu.VMEM(value_cache.shape, bf16),
            pltpu.VMEM((CORES * half // w_key.shape[1], side * side * min(CHUNK, rows), w_key.shape[1]), f32),
            pltpu.VMEM((CORES * half // w_key.shape[1], side * side * min(CHUNK, rows), w_key.shape[1]), f32),
            pltpu.SemaphoreType.DMA((1 + side, dim // depth)),
        ] + sems(64),
        compiler_params=pltpu.CompilerParams(collective_id=0, has_side_effects=True, vmem_limit_bytes=63 << 20),
        name='attend',
    )(lens, hidden, w_query, w_out, w_key, w_value, key_cache, value_cache)


def project_context(side, context, w_a, w_b, hidden):
    rows, depth = context.shape[2:]
    width = w_a.shape[-1]
    bf16, f32 = jnp.bfloat16, jnp.float32
    return pl.pallas_call(
        functools.partial(output_kernel, side),
        out_shape=pltpu.VMEM(hidden.shape, bf16),
        in_specs=[VMEM, ANY, ANY, ANY],
        out_specs=ANY,
        scratch_shapes=[
            pltpu.VMEM((2, side, side, side, rows, depth), bf16),
            pltpu.VMEM((2, side, CORES) + w_a.shape[1:], bf16),
            pltpu.VMEM((2, side, rows, width), f32),
            pltpu.VMEM((2, 2, side // 2, rows, width), f32),
            pltpu.VMEM((2, 4, side, rows, width), bf16),
            pltpu.VMEM((2, 2, side // 2, rows, width), bf16),
            pltpu.VMEM((2, 2, side, rows, width), bf16),
            pltpu.VMEM((2, side, rows, width), bf16),
        ] + sems(128),
        compiler_params=pltpu.CompilerParams(collective_id=1, has_side_effects=True, vmem_limit_bytes=30 << 20),
        name='project_context',
    )(context, w_a, w_b, hidden)


def put_kernel(src_ref, dst_ref, copy_sems):
    n = src_ref.shape[0] * src_ref.shape[1]
    side = src_ref.shape[1]
    copies = [pltpu.make_async_copy(src_ref.at[i // side, i % side], dst_ref.at[i // side, i % side], copy_sems.at[i]) for i in range(n)]
    for copy in copies:
        copy.start()
    for copy in copies:
        copy.wait()


def put(result):
    return pl.pallas_call(
        put_kernel,
        out_shape=jax.ShapeDtypeStruct(result.shape, result.dtype),
        in_specs=[ANY],
        out_specs=ANY,
        scratch_shapes=[pltpu.SemaphoreType.DMA((result.shape[0] * result.shape[1],))],
        compiler_params=pltpu.CompilerParams(vmem_limit_bytes=1 << 20),
        name='put',
    )(result)


def solution(mesh):
    side = math.isqrt(mesh.shape['model'] // CORES)

    def group_step(hidden, w_query, w_key, w_value, w_out, key_cache, value_cache, lengths):
        n_rows, dim = hidden.shape
        local_rows = key_cache.shape[0]
        hidden_tiles = hidden.reshape(side, side, CORES, local_rows, dim)
        w_a, w_b, new, context = attend(side, lengths, hidden_tiles, w_query, w_out, w_key, w_value, key_cache, value_cache)
        key_upd, value_upd = update(lengths, new, key_cache, value_cache)
        result = project_context(side, context, w_a, w_b, hidden_tiles)
        hidden_out = put(result)
        return hidden_out.reshape(n_rows, dim), key_upd, value_upd

    row_spec = P('replica', None)
    cache_spec = P(('replica', 'model'), None, None)
    return jax.shard_map(group_step, mesh=mesh, in_specs=(row_spec, P(None, 'model'), P(None, None), P(None, None), P('model', None), cache_spec, cache_spec, P('replica')), out_specs=(row_spec, cache_spec, cache_spec), check_vma=False)
```

```python
import functools
import math
import jax
import jax.numpy as jnp
from jax import lax
from jax.experimental import pallas as pl
from jax.experimental.pallas import tpu as pltpu
from jax.sharding import PartitionSpec as P

CHUNK = 16


def attend_rows(query, keys, values, new_keys, new_values, row_lens, score_scale):
    positions = lax.broadcasted_iota(jnp.int32, (1, keys[0].shape[0]), 1)
    factor = score_scale * math.log2(math.e)
    old = [
        lax.dot_general(q.astype(jnp.bfloat16), k, (((1,), (1,)), ((), ())), preferred_element_type=jnp.float32) + jnp.where(positions < n, 0.0, -jnp.inf)
        for q, k, n in zip(query, keys, row_lens)
    ]
    own = [jnp.sum(q * k, axis=1, keepdims=True) for q, k in zip(query, new_keys)]
    tops = [jnp.maximum(jnp.max(s, axis=1, keepdims=True), o) for s, o in zip(old, own)]
    old = [jnp.exp2((s - t) * factor) for s, t in zip(old, tops)]
    own = [jnp.exp2((o - t) * factor) for o, t in zip(own, tops)]
    sums = [jnp.sum(s, axis=1, keepdims=True) + o for s, o in zip(old, own)]
    mixed = [jnp.dot(s.astype(jnp.bfloat16), v, preferred_element_type=jnp.float32) for s, v in zip(old, values)]
    return [(m + o.astype(jnp.bfloat16).astype(jnp.float32) * v) / t for m, o, v, t in zip(mixed, own, new_values, sums)]


def update_kernel(len_ref, new_ref, k_ref, v_ref, ko_hbm, vo_hbm, tiles, big_sems, small_sems):
    n, seq_len, head_dim = k_ref.shape
    tile = math.gcd(seq_len, 16)
    first = lax.axis_index('model') * n
    pairs = ((k_ref, ko_hbm), (v_ref, vo_hbm))

    def bulk(i):
        part = pl.ds(i * CHUNK, CHUNK)
        return [pltpu.make_async_copy(src.at[part], dst.at[part], big_sems.at[j, i]) for j, (src, dst) in enumerate(pairs)]

    def start_of(r):
        return pl.multiple_of((len_ref[first + r] // tile) * tile, tile)

    def patches(r):
        return [pltpu.make_async_copy(tiles.at[j, r], dst.at[r, pl.ds(start_of(r), tile)], small_sems.at[j, r]) for j, (_, dst) in enumerate(pairs)]

    for i in range(n // CHUNK):
        for copy in bulk(i):
            copy.start()

    @pl.loop(0, n // CHUNK)
    def _(i):
        for r in range(CHUNK):
            r = i * CHUNK + r
            base = start_of(r)
            pick = lax.broadcasted_iota(jnp.int32, (tile, head_dim), 0) == len_ref[first + r] - base
            for j, (ref, _) in enumerate(pairs):
                new = jnp.broadcast_to(new_ref[j, pl.ds(r, 1), :], (tile, head_dim))
                old = ref[r, pl.ds(base, tile), :].astype(jnp.float32)
                tiles[j, r] = jnp.where(pick, new, old).astype(jnp.bfloat16)

    @pl.loop(0, n // CHUNK)
    def _(i):
        for copy in bulk(i):
            copy.wait()
        for r in range(CHUNK):
            for copy in patches(i * CHUNK + r):
                copy.start()

    @pl.loop(0, n)
    def _(r):
        for copy in patches(r):
            copy.wait()


def update(lens, new, key_cache, value_cache):
    n, seq_len, head_dim = key_cache.shape
    return pl.pallas_call(
        update_kernel,
        in_specs=[pl.BlockSpec(memory_space=pltpu.SMEM), VMEM, VMEM, VMEM],
        out_specs=[ANY] * 2,
        out_shape=[jax.ShapeDtypeStruct(x.shape, x.dtype) for x in (key_cache, value_cache)],
        scratch_shapes=[
            pltpu.VMEM((2, n, math.gcd(seq_len, 16), head_dim), jnp.bfloat16),
            pltpu.SemaphoreType.DMA((2, n // CHUNK)),
            pltpu.SemaphoreType.DMA((2, n)),
        ],
        compiler_params=pltpu.CompilerParams(vmem_limit_bytes=2 << 20),
        name='update',
    )(lens, new, key_cache, value_cache)


ANY = pl.BlockSpec(memory_space=pl.ANY)
VMEM = pl.BlockSpec(memory_space=pltpu.VMEM)


MESH = pl.DeviceIdType.MESH
CORES = 2
EARLY = (2,)


class Moves:
    def __init__(self, send_sems, recv_sems):
        self.send_sems, self.recv_sems = send_sems, recv_sems
        self.count, self.copies, self.unsent = 0, {}, []

    def send(self, key, src, dst, device):
        copy = pltpu.make_async_remote_copy(src_ref=src, dst_ref=dst, send_sem=self.send_sems.at[self.count], recv_sem=self.recv_sems.at[self.count], device_id={'model': device}, device_id_type=MESH)
        copy.start()
        self.count += 1
        self.copies[key] = copy
        self.unsent.append(copy)

    def local(self, key, src, dst):
        copy = pltpu.make_async_copy(src, dst, self.send_sems.at[self.count])
        copy.start()
        self.count += 1
        self.copies[key] = copy

    def got(self, key):
        self.copies.pop(key).wait_recv()

    def done(self, key):
        self.copies.pop(key).wait()

    def finish(self):
        for copy in self.unsent:
            copy.wait_send()


def place(side):
    me = lax.axis_index('model')
    return me // (CORES * side), lax.rem(me // CORES, side), lax.rem(me, CORES)


def greet(devices):
    barrier = pltpu.get_barrier_semaphore()
    for device in devices:
        pl.semaphore_signal(barrier, inc=1, device_id={'model': device}, device_id_type=MESH)
    pl.semaphore_wait(barrier, len(devices))


def columns(start, width):
    return pl.ds(pl.multiple_of(start * width, width), width)


def attend_kernel(side, len_ref, hid_ref, wq_ref, wo_ref, wk_ref, wv_ref, k_hbm, v_hbm, wa_ref, wb_ref, new_ref, ctx_ref, k_ref, v_ref, wq_all, hid, q_buf, q_got, acc, w_new, own_w, q_rows, ctx_rows, load_sems, send_sems, recv_sems):
    y, x, c = place(side)
    rows, dim = hid_ref.shape[3:]
    half = wq_ref.shape[1]
    w_rows = wo_ref.shape[0]
    width = wo_ref.shape[1] // (2 * side)
    w_refs = (wa_ref, wb_ref)
    step = lambda a, d: lax.rem(a + d + side, side)
    dev = lambda yy, xx: (yy * side + xx) * CORES + c
    other = (y * side + x) * CORES + 1 - c
    peers = [(dy, dx) for dy in range(side) for dx in range(side) if dy or dx]
    mv = Moves(send_sems, recv_sems)
    order = list(range(1, side)) + [0]
    depth, piece = min(2048, dim), rows // 2
    halves = [pl.ds(h * piece, piece) for h in range(2)]

    def loads(k):
        part = columns(k, depth)
        pairs = [(wq_ref.at[part], wq_all.at[c, part])] + [(hid_ref.at[step(y, dy), :, c, :, part], hid.at[i, :, :, part]) for i, dy in enumerate(order)]
        return [pltpu.make_async_copy(src, dst, load_sems.at[j, k]) for j, (src, dst) in enumerate(pairs)]

    for k in range(dim // depth):
        for copy in loads(k):
            copy.start()
    greet([dev(step(y, dy), step(x, dx)) for dy, dx in peers] + [other])
    mv.send('wq', wq_ref, wq_all.at[c], other)
    along = ((x, lambda u: dev(y, u)), (y, lambda u: dev(u, x)))
    wcols = lambda t, u: columns(t * side + u, width)
    for t, (u, at) in enumerate(along):
        for d in EARLY:
            mv.send(('w', t, d), wo_ref.at[:, wcols(t, step(u, d))], w_refs[t].at[u], at(step(u, d)))
        mv.local(('w_own', t), wo_ref.at[:, wcols(t, u)], own_w.at[t])
    for j, ref in enumerate((wk_ref, wv_ref)):
        mv.local(('w_new', j), ref, w_new.at[j])
    for j, (src, dst) in enumerate(((k_hbm, k_ref), (v_hbm, v_ref))):
        mv.local(('cache', j), src, dst)

    def gain(h, core, part):
        acc[h] += jnp.dot(hid[:, :, halves[h], part].reshape(side * side * piece, depth), wq_all[core, part, :], preferred_element_type=jnp.float32)

    def store(h, core):
        q_buf[:, :, halves[h], columns(core, half)] = acc[h].astype(jnp.bfloat16).reshape(side, side, piece, half)
        acc[h] = jnp.zeros_like(acc[h])

    acc[...] = jnp.zeros_like(acc)

    @pl.loop(0, dim // depth)
    def _(k):
        for copy in loads(k):
            copy.wait()
        for h in range(2):
            gain(h, c, columns(k, depth))

    for h in range(2):
        store(h, c)

    def project(h):
        @pl.loop(0, dim // depth)
        def _(k):
            gain(h, 1 - c, columns(k, depth))

        store(h, 1 - c)

    for t, (u, at) in enumerate(along):
        mv.done(('w_own', t))
        mv.local(('w_put', t), own_w.at[t], w_refs[t].at[u])
    mv.got('wq')
    for h, some in enumerate(halves):
        project(h)
        for i, dy in enumerate(order):
            for dx in (2, 1, 3, 0):
                if dy or dx:
                    mv.send(('q', dy, dx, h), q_buf.at[i, step(x, dx), some], q_got.at[y, x, some], dev(step(y, dy), step(x, dx)))
                else:
                    q_got[y, x, some] = q_buf[i, x, some]
    for t, (u, at) in enumerate(along):
        for d in range(1, side):
            if d not in EARLY:
                mv.send(('w', t, d), wo_ref.at[:, wcols(t, step(u, d))], w_refs[t].at[u], at(step(u, d)))
    for j in range(2):
        mv.done(('w_new', j))
        new = jnp.zeros((rows, w_new.shape[2]), jnp.float32)
        for k in range(0, dim, depth):
            new += jnp.dot(hid[side - 1, x, :, k:k + depth], w_new[j, k:k + depth, :], preferred_element_type=jnp.float32)
        new_ref[j] = new.astype(jnp.bfloat16).astype(jnp.float32)
        mv.done(('cache', j))

    chips, head_dim = side * side, k_ref.shape[2]
    chunk = min(CHUNK, piece)
    lanes = [slice(h * head_dim, (h + 1) * head_dim) for h in range(CORES * half // head_dim)]
    first = lax.axis_index('model') * rows

    def attend_chunk(i):
        part = pl.ds(pl.multiple_of(i * chunk, chunk), chunk)
        for h, lane in enumerate(lanes):
            q_rows[h] = q_got[:, :, part, lane].astype(jnp.float32).reshape(chips * chunk, head_dim)
        some = [i * chunk + r for r in range(chunk)]
        query = []
        for r in range(chunk):
            query.append(jnp.concatenate([q_rows[h, pl.ds(r, chips, stride=chunk), :] for h in range(len(lanes))], axis=0))
        new_keys, new_values = ([new_ref[j, pl.ds(r, 1), :] for r in some] for j in range(2))
        out = attend_rows(query, [k_ref[r] for r in some], [v_ref[r] for r in some], new_keys, new_values, [len_ref[first + r] for r in some], head_dim ** -0.5)
        for r in range(chunk):
            for h in range(len(lanes)):
                ctx_rows[h, pl.ds(r, chips, stride=chunk), :] = out[r][h * chips:(h + 1) * chips]
        for h, lane in enumerate(lanes):
            ctx_ref[:, :, part, lane] = ctx_rows[h].astype(jnp.bfloat16).reshape(side, side, chunk, head_dim)

    for h in range(2):
        for dy, dx in peers:
            mv.got(('q', dy, dx, h))
        pl.loop(h * piece // chunk, (h + 1) * piece // chunk)(attend_chunk)

    for t in range(2):
        mv.done(('w_put', t))
        for d in range(1, side):
            mv.got(('w', t, d))
    mv.finish()


def output_kernel(side, ctx_ref, wa_ref, wb_ref, hid_ref, out_ref, held, w_buf, acc, keep, part, first, second, final, send_sems, recv_sems):
    y, x, c = place(side)
    rows, depth = ctx_ref.shape[2:]
    width = w_buf.shape[-1]
    step = lambda a, d: lax.rem(a + d + side, side)
    dev = lambda yy, xx: (yy * side + xx) * CORES + c
    other = (y * side + x) * CORES + 1 - c
    spots = ((y, x), (x, y))
    at = lambda t, v, u: dev(v, u) if t == 0 else dev(u, v)
    ctx_of = lambda t, v: ctx_ref.at[v] if t == 0 else ctx_ref.at[:, v]
    greet([dev(y, step(x, d)) for d in range(1, side)] + [dev(step(y, d), x) for d in range(1, side)] + [other])
    mv = Moves(send_sems, recv_sems)
    both = range(2)

    def view(ref, t, v, g, us=None):
        us = slice(None) if us is None else us
        cols = columns(t * side + g, width)
        return ref.at[v, us, c, :, cols] if t == 0 else ref.at[us, v, c, :, cols]

    for t in both:
        v, u = spots[t]
        mv.send(('a', t, 2), ctx_of(t, step(v, 2)), held.at[t, u, v], at(t, step(v, 2), u))
    for t in both:
        v, u = spots[t]
        for d in (1, 3):
            mv.send(('a', t, d), ctx_of(t, step(v, d)), held.at[t, u, v], at(t, step(v, d), u))
        mv.send(('gR', t, 0), ctx_of(t, v), held.at[t, u, v], at(t, v, step(u, 1)))
        mv.send(('gL', t, 0), ctx_of(t, v), held.at[t, u, v], at(t, v, step(u, -1)))
    for t in both:
        v, u = spots[t]
        mv.local(('w', t), (wa_ref, wb_ref)[t], w_buf.at[t, :, c])
        mv.send(('wS', t), (wa_ref, wb_ref)[t], w_buf.at[t, :, c], other)
        mv.local(('hid', t), view(hid_ref, t, v, u), final.at[t])

    def spread(t, p, tag):
        v, u = spots[t]
        slot = held.at[t, u, step(v, -p)]
        mv.send(('g' + tag, t, p), slot, slot, at(t, v, step(u, 1 if tag == 'R' else -1)))

    def forward(t, p, tag):
        v, u = spots[t]
        mv.got(('g' + tag, t, p))
        slot = held.at[t, step(u, -1 if tag == 'R' else 1), step(v, -p)]
        mv.send(('f', t, p), slot, slot, at(t, v, step(u, 1 if tag == 'R' else -1)))

    for t in both:
        mv.got(('a', t, 2))
        spread(t, 2, 'R')
        mv.got(('a', t, 1))
        spread(t, 1, 'L')
        spread(t, 2, 'L')
        spread(t, 1, 'R')
    for t in both:
        forward(t, 2, 'R')
        forward(t, 1, 'L')
        mv.got(('a', t, 3))
        spread(t, 3, 'R')
        spread(t, 3, 'L')
    for t in both:
        forward(t, 0, 'R')
    for t in both:
        mv.done(('w', t))
        mv.got(('wS', t))

    def product(t, p):
        v, u = spots[t]
        total = None
        for k in range(side):
            pieces = []
            for d in range(side):
                if p == 0 and d == 0:
                    pieces.append(ctx_ref[v, k] if t == 0 else ctx_ref[k, v])
                else:
                    pieces.append(held[t, step(u, d), step(v, -p), k])
            one = jnp.dot(jnp.concatenate(pieces, axis=0), w_buf[t, k].reshape(depth, width), preferred_element_type=jnp.float32)
            total = one if total is None else total + one
        acc[t] = total.reshape(side, rows, width)

    upper, lower = pl.ds(0, side // 2), pl.ds(side // 2, side // 2)
    for t in both:
        v, u = spots[t]
        mv.got(('gL', t, 2))
        mv.got(('f', t, 2))
        product(t, 2)
        part[t, 2] = acc[t].astype(jnp.bfloat16)
        mv.send(('r1R', t), part.at[t, 2, upper], first.at[t, 0], at(t, step(v, 1), u))
        mv.send(('r1L', t), part.at[t, 2, lower], first.at[t, 1], at(t, step(v, -1), u))
    for t in both:
        forward(t, 3, 'L')
    sides = ((1, upper, lower, 'L', 1), (3, lower, upper, 'R', 0))
    for p, now, later, tag, d in sides:
        for t in both:
            v, u = spots[t]
            mv.got(('gR', t, p))
            mv.got(('f', t, p))
            product(t, p)
            part[t, p, now] = acc[t, now].astype(jnp.bfloat16)
            mv.send(('r2' + tag, t), part.at[t, p, now], second.at[t, d, now], at(t, step(v, -p), u))
            keep[t, d] = acc[t, later]
    for p, now, later, tag, d in sides:
        for t in both:
            v, u = spots[t]
            mv.got(('r1' + tag, t))
            part[t, p, later] = (keep[t, d] + first[t, d].astype(jnp.float32)).astype(jnp.bfloat16)
            mv.send(('r3' + tag, t), part.at[t, p, later], second.at[t, d, later], at(t, step(v, -p), u))
    for t in both:
        mv.got(('gL', t, 0))
        mv.got(('f', t, 0))
        product(t, 0)
    for t in both:
        v, u = spots[t]
        for tag in 'RL':
            mv.got(('r2' + tag, t))
            mv.got(('r3' + tag, t))
        mv.done(('hid', t))
        for d in range(side):
            us = step(u, d)
            y_sum = acc[t, d] + second[t, 0, d].astype(jnp.float32) + second[t, 1, d].astype(jnp.float32)
            final[t, us] = (final[t, us].astype(jnp.float32) + y_sum).astype(jnp.bfloat16)
        mine = view(out_ref, t, v, u)
        mv.send(('oR', t), final.at[t], mine, at(t, v, step(u, 1)))
        mv.send(('oL', t), final.at[t], mine, at(t, v, step(u, -1)))
        mv.send(('pR', t, 0), final.at[t], mine, at(t, step(v, 1), u))
        mv.send(('pL', t, 0), final.at[t], mine, at(t, step(v, -1), u))
        mv.local(('own', t), final.at[t], mine)
        mv.send(('s', t, 0, 0), final.at[t], mine, other)
    for t in both:
        v, u = spots[t]
        mv.got(('oR', t))
        half = view(out_ref, t, v, step(u, -1), upper)
        mv.send(('o2R', t), half, half, at(t, v, step(u, 1)))
        mv.got(('oL', t))
        half = view(out_ref, t, v, step(u, 1), lower)
        mv.send(('o2L', t), half, half, at(t, v, step(u, -1)))
    offsets = (0, -1, 1, 2)
    for g in (1, 2, 3):
        for t in both:
            v, u = spots[t]
            if g == 3:
                mv.got(('o2R', t))
                mv.got(('o2L', t))
            piece = view(out_ref, t, v, step(u, offsets[g]))
            mv.send(('pR', t, g), piece, piece, at(t, step(v, 1), u))
            mv.send(('pL', t, g), piece, piece, at(t, step(v, -1), u))
            mv.send(('s', t, 0, g), piece, piece, other)
    for g in range(4):
        for t in both:
            v, u = spots[t]
            mv.got(('pR', t, g))
            piece = view(out_ref, t, step(v, -1), step(u, offsets[g]))
            if g in (0, 2):
                mv.send(('z', t, g), piece, piece, at(t, step(v, 1), u))
            mv.send(('s', t, 1, g), piece, piece, other)
            mv.got(('pL', t, g))
            piece = view(out_ref, t, step(v, 1), step(u, offsets[g]))
            if g in (1, 3):
                mv.send(('z', t, g), piece, piece, at(t, step(v, -1), u))
            mv.send(('s', t, 2, g), piece, piece, other)
    for g in range(4):
        for t in both:
            v, u = spots[t]
            mv.got(('z', t, g))
            piece = view(out_ref, t, step(v, 2), step(u, offsets[g]))
            mv.send(('s', t, 3, g), piece, piece, other)
    for t in both:
        mv.done(('own', t))
        for i in range(4):
            for g in range(4):
                mv.got(('s', t, i, g))
    mv.finish()


def sems(n):
    return [pltpu.SemaphoreType.DMA((n,)), pltpu.SemaphoreType.DMA((n,))]


def attend(side, lens, hidden, w_query, w_out, w_key, w_value, key_cache, value_cache):
    rows, dim = hidden.shape[3:]
    half = w_query.shape[1]
    w_rows, width = w_out.shape[0], w_out.shape[1] // (2 * side)
    bf16, f32 = jnp.bfloat16, jnp.float32
    tile = jax.ShapeDtypeStruct((side, w_rows, width), bf16)
    wide = (side, side, rows, CORES * half)
    depth = min(2048, dim)
    return pl.pallas_call(
        functools.partial(attend_kernel, side),
        out_shape=[tile, tile, jax.ShapeDtypeStruct((2, rows, w_key.shape[1]), f32), jax.ShapeDtypeStruct(wide, bf16), pltpu.VMEM(key_cache.shape, bf16), pltpu.VMEM(value_cache.shape, bf16)],
        in_specs=[pl.BlockSpec(memory_space=pltpu.SMEM)] + [ANY] * 7,
        out_specs=[ANY, ANY, VMEM, VMEM, VMEM, VMEM],
        scratch_shapes=[
            pltpu.VMEM((CORES, dim, half), bf16),
            pltpu.VMEM((side, side, rows, dim), bf16),
            pltpu.VMEM(wide, bf16),
            pltpu.VMEM(wide, bf16),
            pltpu.VMEM((2, side // 2 * side * rows, half), f32),
            pltpu.VMEM((2,) + w_key.shape, bf16),
            pltpu.VMEM((2, w_rows, width), bf16),
            pltpu.VMEM((CORES * half // w_key.shape[1], side * side * min(CHUNK, rows // 2), w_key.shape[1]), f32),
            pltpu.VMEM((CORES * half // w_key.shape[1], side * side * min(CHUNK, rows // 2), w_key.shape[1]), f32),
            pltpu.SemaphoreType.DMA((1 + side, dim // depth)),
        ] + sems(64),
        compiler_params=pltpu.CompilerParams(collective_id=0, has_side_effects=True, vmem_limit_bytes=40 << 20),
        name='attend',
    )(lens, hidden, w_query, w_out, w_key, w_value, key_cache, value_cache)


def project_context(side, context, w_a, w_b, hidden):
    rows, depth = context.shape[2:]
    width = w_a.shape[-1]
    bf16, f32 = jnp.bfloat16, jnp.float32
    return pl.pallas_call(
        functools.partial(output_kernel, side),
        out_shape=pltpu.VMEM(hidden.shape, bf16),
        in_specs=[VMEM, ANY, ANY, ANY],
        out_specs=ANY,
        scratch_shapes=[
            pltpu.VMEM((2, side, side, side, rows, depth), bf16),
            pltpu.VMEM((2, side, CORES) + w_a.shape[1:], bf16),
            pltpu.VMEM((2, side, rows, width), f32),
            pltpu.VMEM((2, 2, side // 2, rows, width), f32),
            pltpu.VMEM((2, 4, side, rows, width), bf16),
            pltpu.VMEM((2, 2, side // 2, rows, width), bf16),
            pltpu.VMEM((2, 2, side, rows, width), bf16),
            pltpu.VMEM((2, side, rows, width), bf16),
        ] + sems(128),
        compiler_params=pltpu.CompilerParams(collective_id=1, has_side_effects=True, vmem_limit_bytes=30 << 20),
        name='project_context',
    )(context, w_a, w_b, hidden)


def put_kernel(src_ref, dst_ref, copy_sems):
    n = src_ref.shape[0] * src_ref.shape[1]
    side = src_ref.shape[1]
    copies = [pltpu.make_async_copy(src_ref.at[i // side, i % side], dst_ref.at[i // side, i % side], copy_sems.at[i]) for i in range(n)]
    for copy in copies:
        copy.start()
    for copy in copies:
        copy.wait()


def put(result):
    return pl.pallas_call(
        put_kernel,
        out_shape=jax.ShapeDtypeStruct(result.shape, result.dtype),
        in_specs=[ANY],
        out_specs=ANY,
        scratch_shapes=[pltpu.SemaphoreType.DMA((result.shape[0] * result.shape[1],))],
        compiler_params=pltpu.CompilerParams(vmem_limit_bytes=1 << 20),
        name='put',
    )(result)


def solution(mesh):
    side = math.isqrt(mesh.shape['model'] // CORES)

    def group_step(hidden, w_query, w_key, w_value, w_out, key_cache, value_cache, lengths):
        n_rows, dim = hidden.shape
        local_rows = key_cache.shape[0]
        hidden_tiles = hidden.reshape(side, side, CORES, local_rows, dim)
        w_a, w_b, new, context, keys, values = attend(side, lengths, hidden_tiles, w_query, w_out, w_key, w_value, key_cache, value_cache)
        key_upd, value_upd = update(lengths, new, keys, values)
        context, key_upd, value_upd = lax.optimization_barrier((context, key_upd, value_upd))
        result = project_context(side, context, w_a, w_b, hidden_tiles)
        hidden_out = put(result)
        return hidden_out.reshape(n_rows, dim), key_upd, value_upd

    row_spec = P('replica', None)
    cache_spec = P(('replica', 'model'), None, None)
    return jax.shard_map(group_step, mesh=mesh, in_specs=(row_spec, P(None, 'model'), P(None, None), P(None, None), P('model', None), cache_spec, cache_spec, P('replica')), out_specs=(row_spec, cache_spec, cache_spec), check_vma=False)
```

```python
import functools
import math
import jax
import jax.numpy as jnp
from jax import lax
from jax.experimental import pallas as pl
from jax.experimental.pallas import tpu as pltpu
from jax.sharding import PartitionSpec as P

CHUNK = 16


def attend_rows(query, keys, values, new_keys, new_values, row_lens, score_scale):
    positions = lax.broadcasted_iota(jnp.int32, (1, keys[0].shape[0]), 1)
    factor = score_scale * math.log2(math.e)
    old = [
        lax.dot_general(q.astype(jnp.bfloat16), k, (((1,), (1,)), ((), ())), preferred_element_type=jnp.float32) + jnp.where(positions < n, 0.0, -jnp.inf)
        for q, k, n in zip(query, keys, row_lens)
    ]
    own = [jnp.sum(q * k, axis=1, keepdims=True) for q, k in zip(query, new_keys)]
    tops = [jnp.maximum(jnp.max(s, axis=1, keepdims=True), o) for s, o in zip(old, own)]
    old = [jnp.exp2((s - t) * factor) for s, t in zip(old, tops)]
    own = [jnp.exp2((o - t) * factor) for o, t in zip(own, tops)]
    sums = [jnp.sum(s, axis=1, keepdims=True) + o for s, o in zip(old, own)]
    mixed = [jnp.dot(s.astype(jnp.bfloat16), v, preferred_element_type=jnp.float32) for s, v in zip(old, values)]
    return [(m + o.astype(jnp.bfloat16).astype(jnp.float32) * v) / t for m, o, v, t in zip(mixed, own, new_values, sums)]


def update_kernel(len_ref, new_ref, k_ref, v_ref, ko_hbm, vo_hbm, tiles, big_sems, small_sems):
    n, seq_len, head_dim = k_ref.shape
    tile = math.gcd(seq_len, 16)
    first = lax.axis_index('model') * n
    pairs = ((k_ref, ko_hbm), (v_ref, vo_hbm))

    def bulk(i):
        part = pl.ds(i * CHUNK, CHUNK)
        return [pltpu.make_async_copy(src.at[part], dst.at[part], big_sems.at[j, i]) for j, (src, dst) in enumerate(pairs)]

    def start_of(r):
        return pl.multiple_of((len_ref[first + r] // tile) * tile, tile)

    def patches(r):
        return [pltpu.make_async_copy(tiles.at[j, r], dst.at[r, pl.ds(start_of(r), tile)], small_sems.at[j, r]) for j, (_, dst) in enumerate(pairs)]

    for i in range(n // CHUNK):
        for copy in bulk(i):
            copy.start()

    @pl.loop(0, n // CHUNK)
    def _(i):
        for r in range(CHUNK):
            r = i * CHUNK + r
            base = start_of(r)
            pick = lax.broadcasted_iota(jnp.int32, (tile, head_dim), 0) == len_ref[first + r] - base
            for j, (ref, _) in enumerate(pairs):
                new = jnp.broadcast_to(new_ref[j, pl.ds(r, 1), :], (tile, head_dim))
                old = ref[r, pl.ds(base, tile), :].astype(jnp.float32)
                tiles[j, r] = jnp.where(pick, new, old).astype(jnp.bfloat16)

    @pl.loop(0, n // CHUNK)
    def _(i):
        for copy in bulk(i):
            copy.wait()
        for r in range(CHUNK):
            for copy in patches(i * CHUNK + r):
                copy.start()

    @pl.loop(0, n)
    def _(r):
        for copy in patches(r):
            copy.wait()


def update(lens, new, key_cache, value_cache):
    n, seq_len, head_dim = key_cache.shape
    return pl.pallas_call(
        update_kernel,
        in_specs=[pl.BlockSpec(memory_space=pltpu.SMEM), VMEM, VMEM, VMEM],
        out_specs=[ANY] * 2,
        out_shape=[jax.ShapeDtypeStruct(x.shape, x.dtype) for x in (key_cache, value_cache)],
        scratch_shapes=[
            pltpu.VMEM((2, n, math.gcd(seq_len, 16), head_dim), jnp.bfloat16),
            pltpu.SemaphoreType.DMA((2, n // CHUNK)),
            pltpu.SemaphoreType.DMA((2, n)),
        ],
        compiler_params=pltpu.CompilerParams(vmem_limit_bytes=2 << 20),
        name='update',
    )(lens, new, key_cache, value_cache)


ANY = pl.BlockSpec(memory_space=pl.ANY)
VMEM = pl.BlockSpec(memory_space=pltpu.VMEM)


MESH = pl.DeviceIdType.MESH
CORES = 2


class Moves:
    def __init__(self, send_sems, recv_sems):
        self.send_sems, self.recv_sems = send_sems, recv_sems
        self.count, self.copies, self.unsent = 0, {}, []

    def send(self, key, src, dst, device):
        copy = pltpu.make_async_remote_copy(src_ref=src, dst_ref=dst, send_sem=self.send_sems.at[self.count], recv_sem=self.recv_sems.at[self.count], device_id={'model': device}, device_id_type=MESH)
        copy.start()
        self.count += 1
        self.copies[key] = copy
        self.unsent.append(copy)

    def local(self, key, src, dst):
        copy = pltpu.make_async_copy(src, dst, self.send_sems.at[self.count])
        copy.start()
        self.count += 1
        self.copies[key] = copy

    def got(self, key):
        self.copies.pop(key).wait_recv()

    def done(self, key):
        self.copies.pop(key).wait()

    def finish(self):
        for copy in self.unsent:
            copy.wait_send()


def place(side):
    me = lax.axis_index('model')
    return me // (CORES * side), lax.rem(me // CORES, side), lax.rem(me, CORES)


def greet(devices):
    barrier = pltpu.get_barrier_semaphore()
    for device in devices:
        pl.semaphore_signal(barrier, inc=1, device_id={'model': device}, device_id_type=MESH)
    pl.semaphore_wait(barrier, len(devices))


def columns(start, width):
    return pl.ds(pl.multiple_of(start * width, width), width)


def attend_kernel(side, len_ref, hid_ref, wq_ref, wo_ref, wk_ref, wv_ref, k_hbm, v_hbm, wa_ref, wb_ref, new_ref, ctx_ref, k_ref, v_ref, wq_all, hid, q_buf, q_got, acc, relay, w_new, own_w, q_rows, ctx_rows, load_sems, send_sems, recv_sems):
    y, x, c = place(side)
    rows, dim = hid_ref.shape[3:]
    half = wq_ref.shape[1]
    w_rows = wo_ref.shape[0]
    width = wo_ref.shape[1] // (2 * side)
    w_refs = (wa_ref, wb_ref)
    step = lambda a, d: lax.rem(a + d + side, side)
    dev = lambda yy, xx: (yy * side + xx) * CORES + c
    other = (y * side + x) * CORES + 1 - c
    peers = [(dy, dx) for dy in range(side) for dx in range(side) if dy or dx]
    mv = Moves(send_sems, recv_sems)
    order = list(range(1, side)) + [0]
    depth, piece = min(2048, dim), rows // 2
    halves = [pl.ds(h * piece, piece) for h in range(2)]

    def loads(k):
        part = columns(k, depth)
        pairs = [(wq_ref.at[part], wq_all.at[c, part])] + [(hid_ref.at[step(y, dy), :, c, :, part], hid.at[i, :, :, part]) for i, dy in enumerate(order)]
        return [pltpu.make_async_copy(src, dst, load_sems.at[j, k]) for j, (src, dst) in enumerate(pairs)]

    for k in range(dim // depth):
        for copy in loads(k):
            copy.start()
    greet([dev(step(y, dy), step(x, dx)) for dy, dx in peers] + [other])
    mv.send('wq', wq_ref, wq_all.at[c], other)
    along = ((x, lambda u: dev(y, u)), (y, lambda u: dev(u, x)))
    wcols = lambda t, u: columns(t * side + u, width)
    top, low = pl.ds(0, w_rows // 2), pl.ds(w_rows // 2, w_rows // 2)
    for t, (u, at) in enumerate(along):
        mv.send(('w1R', t), wo_ref.at[top, wcols(t, step(u, 2))], relay.at[t, 0], at(step(u, 1)))
        mv.send(('w1L', t), wo_ref.at[low, wcols(t, step(u, 2))], relay.at[t, 1], at(step(u, -1)))
        mv.local(('w_own', t), wo_ref.at[:, wcols(t, u)], own_w.at[t])
    for j, ref in enumerate((wk_ref, wv_ref)):
        mv.local(('w_new', j), ref, w_new.at[j])
    for j, (src, dst) in enumerate(((k_hbm, k_ref), (v_hbm, v_ref))):
        mv.local(('cache', j), src, dst)

    def gain(h, core, part):
        acc[h] += jnp.dot(hid[:, :, halves[h], part].reshape(side * side * piece, depth), wq_all[core, part, :], preferred_element_type=jnp.float32)

    def store(h, core):
        q_buf[:, :, halves[h], columns(core, half)] = acc[h].astype(jnp.bfloat16).reshape(side, side, piece, half)
        acc[h] = jnp.zeros_like(acc[h])

    acc[...] = jnp.zeros_like(acc)

    @pl.loop(0, dim // depth)
    def _(k):
        for copy in loads(k):
            copy.wait()
        for h in range(2):
            gain(h, c, columns(k, depth))

    for h in range(2):
        store(h, c)

    def project(h):
        @pl.loop(0, dim // depth)
        def _(k):
            gain(h, 1 - c, columns(k, depth))

        store(h, 1 - c)

    for t, (u, at) in enumerate(along):
        mv.done(('w_own', t))
        mv.local(('w_put', t), own_w.at[t], w_refs[t].at[u])
        mv.got(('w1R', t))
        mv.send(('w2R', t), relay.at[t, 0], w_refs[t].at[step(u, -1), top], at(step(u, 1)))
        mv.got(('w1L', t))
        mv.send(('w2L', t), relay.at[t, 1], w_refs[t].at[step(u, 1), low], at(step(u, -1)))
    mv.got('wq')
    for h, some in enumerate(halves):
        project(h)
        for i, dy in enumerate(order):
            for dx in (2, 1, 3, 0):
                if dy or dx:
                    mv.send(('q', dy, dx, h), q_buf.at[i, step(x, dx), some], q_got.at[y, x, some], dev(step(y, dy), step(x, dx)))
                else:
                    q_got[y, x, some] = q_buf[i, x, some]
    for t, (u, at) in enumerate(along):
        for d in (1, 3):
            mv.send(('w', t, d), wo_ref.at[:, wcols(t, step(u, d))], w_refs[t].at[u], at(step(u, d)))
    for j in range(2):
        mv.done(('w_new', j))
        new = jnp.zeros((rows, w_new.shape[2]), jnp.float32)
        for k in range(0, dim, depth):
            new += jnp.dot(hid[side - 1, x, :, k:k + depth], w_new[j, k:k + depth, :], preferred_element_type=jnp.float32)
        new_ref[j] = new.astype(jnp.bfloat16).astype(jnp.float32)
        mv.done(('cache', j))

    chips, head_dim = side * side, k_ref.shape[2]
    chunk = min(CHUNK, piece)
    lanes = [slice(h * head_dim, (h + 1) * head_dim) for h in range(CORES * half // head_dim)]
    first = lax.axis_index('model') * rows

    def attend_chunk(i):
        part = pl.ds(pl.multiple_of(i * chunk, chunk), chunk)
        for h, lane in enumerate(lanes):
            q_rows[h] = q_got[:, :, part, lane].astype(jnp.float32).reshape(chips * chunk, head_dim)
        some = [i * chunk + r for r in range(chunk)]
        query = []
        for r in range(chunk):
            query.append(jnp.concatenate([q_rows[h, pl.ds(r, chips, stride=chunk), :] for h in range(len(lanes))], axis=0))
        new_keys, new_values = ([new_ref[j, pl.ds(r, 1), :] for r in some] for j in range(2))
        out = attend_rows(query, [k_ref[r] for r in some], [v_ref[r] for r in some], new_keys, new_values, [len_ref[first + r] for r in some], head_dim ** -0.5)
        for r in range(chunk):
            for h in range(len(lanes)):
                ctx_rows[h, pl.ds(r, chips, stride=chunk), :] = out[r][h * chips:(h + 1) * chips]
        for h, lane in enumerate(lanes):
            ctx_ref[:, :, part, lane] = ctx_rows[h].astype(jnp.bfloat16).reshape(side, side, chunk, head_dim)

    for h in range(2):
        for dy, dx in peers:
            mv.got(('q', dy, dx, h))
        pl.loop(h * piece // chunk, (h + 1) * piece // chunk)(attend_chunk)

    for t in range(2):
        mv.done(('w_put', t))
        for key in (('w2R', t), ('w2L', t), ('w', t, 1), ('w', t, 3)):
            mv.got(key)
    mv.finish()


def output_kernel(side, ctx_ref, wa_ref, wb_ref, hid_ref, out_ref, held, w_buf, acc, keep, part, first, second, final, send_sems, recv_sems):
    y, x, c = place(side)
    rows, depth = ctx_ref.shape[2:]
    width = w_buf.shape[-1]
    step = lambda a, d: lax.rem(a + d + side, side)
    dev = lambda yy, xx: (yy * side + xx) * CORES + c
    other = (y * side + x) * CORES + 1 - c
    spots = ((y, x), (x, y))
    at = lambda t, v, u: dev(v, u) if t == 0 else dev(u, v)
    ctx_of = lambda t, v: ctx_ref.at[v] if t == 0 else ctx_ref.at[:, v]
    greet([dev(y, step(x, d)) for d in range(1, side)] + [dev(step(y, d), x) for d in range(1, side)] + [other])
    mv = Moves(send_sems, recv_sems)
    both = range(2)

    def view(ref, t, v, g, us=None):
        us = slice(None) if us is None else us
        cols = columns(t * side + g, width)
        return ref.at[v, us, c, :, cols] if t == 0 else ref.at[us, v, c, :, cols]

    for t in both:
        v, u = spots[t]
        mv.send(('a', t, 2), ctx_of(t, step(v, 2)), held.at[t, u, v], at(t, step(v, 2), u))
    for t in both:
        v, u = spots[t]
        for d in (1, 3):
            mv.send(('a', t, d), ctx_of(t, step(v, d)), held.at[t, u, v], at(t, step(v, d), u))
        mv.send(('gR', t, 0), ctx_of(t, v), held.at[t, u, v], at(t, v, step(u, 1)))
        mv.send(('gL', t, 0), ctx_of(t, v), held.at[t, u, v], at(t, v, step(u, -1)))
    for t in both:
        v, u = spots[t]
        mv.local(('w', t), (wa_ref, wb_ref)[t], w_buf.at[t, :, c])
        mv.send(('wS', t), (wa_ref, wb_ref)[t], w_buf.at[t, :, c], other)
        mv.local(('hid', t), view(hid_ref, t, v, u), final.at[t])

    def spread(t, p, tag):
        v, u = spots[t]
        slot = held.at[t, u, step(v, -p)]
        mv.send(('g' + tag, t, p), slot, slot, at(t, v, step(u, 1 if tag == 'R' else -1)))

    def forward(t, p, tag):
        v, u = spots[t]
        mv.got(('g' + tag, t, p))
        slot = held.at[t, step(u, -1 if tag == 'R' else 1), step(v, -p)]
        mv.send(('f', t, p), slot, slot, at(t, v, step(u, 1 if tag == 'R' else -1)))

    for t in both:
        mv.got(('a', t, 2))
        spread(t, 2, 'R')
        mv.got(('a', t, 1))
        spread(t, 1, 'L')
        spread(t, 2, 'L')
        spread(t, 1, 'R')
    for t in both:
        forward(t, 2, 'R')
        forward(t, 1, 'L')
        mv.got(('a', t, 3))
        spread(t, 3, 'R')
        spread(t, 3, 'L')
    for t in both:
        forward(t, 0, 'R')
    for t in both:
        mv.done(('w', t))
        mv.got(('wS', t))

    def product(t, p):
        v, u = spots[t]
        total = None
        for k in range(side):
            pieces = []
            for d in range(side):
                if p == 0 and d == 0:
                    pieces.append(ctx_ref[v, k] if t == 0 else ctx_ref[k, v])
                else:
                    pieces.append(held[t, step(u, d), step(v, -p), k])
            one = jnp.dot(jnp.concatenate(pieces, axis=0), w_buf[t, k].reshape(depth, width), preferred_element_type=jnp.float32)
            total = one if total is None else total + one
        acc[t] = total.reshape(side, rows, width)

    upper, lower = pl.ds(0, side // 2), pl.ds(side // 2, side // 2)
    for t in both:
        v, u = spots[t]
        mv.got(('gL', t, 2))
        mv.got(('f', t, 2))
        product(t, 2)
        part[t, 2] = acc[t].astype(jnp.bfloat16)
        mv.send(('r1R', t), part.at[t, 2, upper], first.at[t, 0], at(t, step(v, 1), u))
        mv.send(('r1L', t), part.at[t, 2, lower], first.at[t, 1], at(t, step(v, -1), u))
    for t in both:
        forward(t, 3, 'L')
    sides = ((1, upper, lower, 'L', 1), (3, lower, upper, 'R', 0))
    for p, now, later, tag, d in sides:
        for t in both:
            v, u = spots[t]
            mv.got(('gR', t, p))
            mv.got(('f', t, p))
            product(t, p)
            part[t, p, now] = acc[t, now].astype(jnp.bfloat16)
            mv.send(('r2' + tag, t), part.at[t, p, now], second.at[t, d, now], at(t, step(v, -p), u))
            keep[t, d] = acc[t, later]
    for p, now, later, tag, d in sides:
        for t in both:
            v, u = spots[t]
            mv.got(('r1' + tag, t))
            part[t, p, later] = (keep[t, d] + first[t, d].astype(jnp.float32)).astype(jnp.bfloat16)
            mv.send(('r3' + tag, t), part.at[t, p, later], second.at[t, d, later], at(t, step(v, -p), u))
    for t in both:
        mv.got(('gL', t, 0))
        mv.got(('f', t, 0))
        product(t, 0)
    for t in both:
        v, u = spots[t]
        for tag in 'RL':
            mv.got(('r2' + tag, t))
            mv.got(('r3' + tag, t))
        mv.done(('hid', t))
        for d in range(side):
            us = step(u, d)
            y_sum = acc[t, d] + second[t, 0, d].astype(jnp.float32) + second[t, 1, d].astype(jnp.float32)
            final[t, us] = (final[t, us].astype(jnp.float32) + y_sum).astype(jnp.bfloat16)
        mine = view(out_ref, t, v, u)
        mv.send(('oR', t), final.at[t], mine, at(t, v, step(u, 1)))
        mv.send(('oL', t), final.at[t], mine, at(t, v, step(u, -1)))
        mv.send(('pR', t, 0), final.at[t], mine, at(t, step(v, 1), u))
        mv.send(('pL', t, 0), final.at[t], mine, at(t, step(v, -1), u))
        mv.local(('own', t), final.at[t], mine)
        mv.send(('s', t, 0, 0), final.at[t], mine, other)
    for t in both:
        v, u = spots[t]
        mv.got(('oR', t))
        half = view(out_ref, t, v, step(u, -1), upper)
        mv.send(('o2R', t), half, half, at(t, v, step(u, 1)))
        mv.got(('oL', t))
        half = view(out_ref, t, v, step(u, 1), lower)
        mv.send(('o2L', t), half, half, at(t, v, step(u, -1)))
    offsets = (0, -1, 1, 2)
    for g in (1, 2, 3):
        for t in both:
            v, u = spots[t]
            if g == 3:
                mv.got(('o2R', t))
                mv.got(('o2L', t))
            piece = view(out_ref, t, v, step(u, offsets[g]))
            mv.send(('pR', t, g), piece, piece, at(t, step(v, 1), u))
            mv.send(('pL', t, g), piece, piece, at(t, step(v, -1), u))
            mv.send(('s', t, 0, g), piece, piece, other)
    for g in range(4):
        for t in both:
            v, u = spots[t]
            mv.got(('pR', t, g))
            piece = view(out_ref, t, step(v, -1), step(u, offsets[g]))
            if g in (0, 2):
                mv.send(('z', t, g), piece, piece, at(t, step(v, 1), u))
            mv.send(('s', t, 1, g), piece, piece, other)
            mv.got(('pL', t, g))
            piece = view(out_ref, t, step(v, 1), step(u, offsets[g]))
            if g in (1, 3):
                mv.send(('z', t, g), piece, piece, at(t, step(v, -1), u))
            mv.send(('s', t, 2, g), piece, piece, other)
    for g in range(4):
        for t in both:
            v, u = spots[t]
            mv.got(('z', t, g))
            piece = view(out_ref, t, step(v, 2), step(u, offsets[g]))
            mv.send(('s', t, 3, g), piece, piece, other)
    for t in both:
        mv.done(('own', t))
        for i in range(4):
            for g in range(4):
                mv.got(('s', t, i, g))
    mv.finish()


def sems(n):
    return [pltpu.SemaphoreType.DMA((n,)), pltpu.SemaphoreType.DMA((n,))]


def attend(side, lens, hidden, w_query, w_out, w_key, w_value, key_cache, value_cache):
    rows, dim = hidden.shape[3:]
    half = w_query.shape[1]
    w_rows, width = w_out.shape[0], w_out.shape[1] // (2 * side)
    bf16, f32 = jnp.bfloat16, jnp.float32
    tile = jax.ShapeDtypeStruct((side, w_rows, width), bf16)
    wide = (side, side, rows, CORES * half)
    depth = min(2048, dim)
    return pl.pallas_call(
        functools.partial(attend_kernel, side),
        out_shape=[tile, tile, jax.ShapeDtypeStruct((2, rows, w_key.shape[1]), f32), jax.ShapeDtypeStruct(wide, bf16), pltpu.VMEM(key_cache.shape, bf16), pltpu.VMEM(value_cache.shape, bf16)],
        in_specs=[pl.BlockSpec(memory_space=pltpu.SMEM)] + [ANY] * 7,
        out_specs=[ANY, ANY, VMEM, VMEM, VMEM, VMEM],
        scratch_shapes=[
            pltpu.VMEM((CORES, dim, half), bf16),
            pltpu.VMEM((side, side, rows, dim), bf16),
            pltpu.VMEM(wide, bf16),
            pltpu.VMEM(wide, bf16),
            pltpu.VMEM((2, side // 2 * side * rows, half), f32),
            pltpu.VMEM((2, 2, w_rows // 2, width), bf16),
            pltpu.VMEM((2,) + w_key.shape, bf16),
            pltpu.VMEM((2, w_rows, width), bf16),
            pltpu.VMEM((CORES * half // w_key.shape[1], side * side * min(CHUNK, rows // 2), w_key.shape[1]), f32),
            pltpu.VMEM((CORES * half // w_key.shape[1], side * side * min(CHUNK, rows // 2), w_key.shape[1]), f32),
            pltpu.SemaphoreType.DMA((1 + side, dim // depth)),
        ] + sems(64),
        compiler_params=pltpu.CompilerParams(collective_id=0, has_side_effects=True, vmem_limit_bytes=40 << 20),
        name='attend',
    )(lens, hidden, w_query, w_out, w_key, w_value, key_cache, value_cache)


def project_context(side, context, w_a, w_b, hidden):
    rows, depth = context.shape[2:]
    width = w_a.shape[-1]
    bf16, f32 = jnp.bfloat16, jnp.float32
    return pl.pallas_call(
        functools.partial(output_kernel, side),
        out_shape=pltpu.VMEM(hidden.shape, bf16),
        in_specs=[VMEM, ANY, ANY, ANY],
        out_specs=ANY,
        scratch_shapes=[
            pltpu.VMEM((2, side, side, side, rows, depth), bf16),
            pltpu.VMEM((2, side, CORES) + w_a.shape[1:], bf16),
            pltpu.VMEM((2, side, rows, width), f32),
            pltpu.VMEM((2, 2, side // 2, rows, width), f32),
            pltpu.VMEM((2, 4, side, rows, width), bf16),
            pltpu.VMEM((2, 2, side // 2, rows, width), bf16),
            pltpu.VMEM((2, 2, side, rows, width), bf16),
            pltpu.VMEM((2, side, rows, width), bf16),
        ] + sems(128),
        compiler_params=pltpu.CompilerParams(collective_id=1, has_side_effects=True, vmem_limit_bytes=30 << 20),
        name='project_context',
    )(context, w_a, w_b, hidden)


def put_kernel(src_ref, dst_ref, copy_sems):
    n = src_ref.shape[0] * src_ref.shape[1]
    side = src_ref.shape[1]
    copies = [pltpu.make_async_copy(src_ref.at[i // side, i % side], dst_ref.at[i // side, i % side], copy_sems.at[i]) for i in range(n)]
    for copy in copies:
        copy.start()
    for copy in copies:
        copy.wait()


def put(result):
    return pl.pallas_call(
        put_kernel,
        out_shape=jax.ShapeDtypeStruct(result.shape, result.dtype),
        in_specs=[ANY],
        out_specs=ANY,
        scratch_shapes=[pltpu.SemaphoreType.DMA((result.shape[0] * result.shape[1],))],
        compiler_params=pltpu.CompilerParams(vmem_limit_bytes=1 << 20),
        name='put',
    )(result)


def solution(mesh):
    side = math.isqrt(mesh.shape['model'] // CORES)

    def group_step(hidden, w_query, w_key, w_value, w_out, key_cache, value_cache, lengths):
        n_rows, dim = hidden.shape
        local_rows = key_cache.shape[0]
        hidden_tiles = hidden.reshape(side, side, CORES, local_rows, dim)
        w_a, w_b, new, context, keys, values = attend(side, lengths, hidden_tiles, w_query, w_out, w_key, w_value, key_cache, value_cache)
        key_upd, value_upd = update(lengths, new, keys, values)
        context, key_upd, value_upd = lax.optimization_barrier((context, key_upd, value_upd))
        result = project_context(side, context, w_a, w_b, hidden_tiles)
        hidden_out = put(result)
        return hidden_out.reshape(n_rows, dim), key_upd, value_upd

    row_spec = P('replica', None)
    cache_spec = P(('replica', 'model'), None, None)
    return jax.shard_map(group_step, mesh=mesh, in_specs=(row_spec, P(None, 'model'), P(None, None), P(None, None), P('model', None), cache_spec, cache_spec, P('replica')), out_specs=(row_spec, cache_spec, cache_spec), check_vma=False)
```
